128 devices in a mesh: py: 8 (over y, core), px: 4 (over x), pz: 4 (over z).
Axes of the slice: x: 4, y: 4, z: 4, core: 2. Of those that a mesh axis runs over, the one named last changes fastest.
Arguments:
- tracer: float32 [128, 512, 32, 128], P('py', 'px', 'pz'), may hold values from 0.2 to 1.8
- conductance: float32 [128, 512, 32, 128], P('py', 'px', 'pz'), may hold values from 0.03 to 0.15
- source: float32 [128, 512, 32, 128], P('py', 'px', 'pz'), may hold values from -0.2 to 0.2
Outputs:
- potential: float32 [128, 512, 32, 128], P('py', 'px', 'pz')
- tracer_end: float32 [128, 512, 32, 128], P('py', 'px', 'pz')
The draws below stay inside these ranges and needn't reach their ends.
All inputs are finite; a program needn't handle non-finite values.
Results may differ from the reference program's by a relative error of at most 0.00002.
Values sent between devices are 32-bit elements; how exact they have to be, the bound alone decides.
A program may use at most 320 MiB of HBM per device.

```python
import jax
import jax.numpy as jnp
from jax import lax

GRID_Y = 128
GRID_X = 512
GRID_Z = 32
MEMBERS = 128
STEPS = 4


def block_scale(stream_key, shape, shards, least, high):
    factor_of = 1.0
    for position, parts in shards:
        draws = jax.random.uniform(jax.random.fold_in(jax.random.fold_in(stream_key, 6), position), (parts,), jnp.float32, least / len(shards), high / len(shards))
        factor_of = factor_of * jnp.repeat(jnp.exp(draws), shape[position] // parts).reshape((-1,) + (1,) * (len(shape) - 1 - position))
    return factor_of


def setup_inputs(seed: int = 0) -> dict:
    splits = jax.random.split(jax.random.key(seed), 4)
    tracer = jnp.clip(0.2 + 1.5999999 * jax.random.uniform(splits[0], (GRID_Y, GRID_X, GRID_Z, MEMBERS), jnp.float32) ** block_scale(splits[0], (GRID_Y, GRID_X, GRID_Z, MEMBERS), ((0, 8), (1, 4), (2, 4)), -0.2, 0.2), 0.2, 1.8)
    conductance = jnp.clip(0.03 + 0.120000007 * jax.random.uniform(splits[1], (GRID_Y, GRID_X, GRID_Z, MEMBERS), jnp.float32) ** block_scale(splits[1], (GRID_Y, GRID_X, GRID_Z, MEMBERS), ((0, 8), (1, 4), (2, 4)), -0.2, 0.2), 0.03, 0.15)
    source = jnp.clip(jax.random.uniform(splits[2], (GRID_Y, GRID_X, GRID_Z, MEMBERS), jnp.float32, -0.2, 0.2) * block_scale(splits[2], (GRID_Y, GRID_X, GRID_Z, MEMBERS), ((0, 8), (1, 4), (2, 4)), -0.4, 0.0), -0.2, 0.2)
    return dict(tracer=tracer, conductance=conductance, source=source)


def strip_edges(values, dims):
    for dim in dims:
        values = lax.slice_in_dim(values, 1, values.shape[dim] - 1, axis=dim)
    return values


def neighbour(values, dim, start, dims):
    others = [other for other in dims if other != dim]
    values = strip_edges(values, others)
    return lax.slice_in_dim(values, start, start + values.shape[dim] - 2, axis=dim)


def one_step(padded, conductance, source):
    middle = strip_edges(padded, (0, 1, 2))
    lower = [neighbour(padded, dim, 0, (0, 1, 2)) for dim in (0, 1, 2)]
    upper = [neighbour(padded, dim, 2, (0, 1, 2)) for dim in (0, 1, 2)]
    spread = lower[0] + upper[0] + lower[1] + upper[1] + lower[2] + upper[2] - 6.0 * middle
    return middle + conductance * spread + source


def reference(tracer, conductance, source):
    for step in range(STEPS):
        tracer = one_step(jnp.pad(tracer, ((1, 1), (1, 1), (1, 1), (0, 0)), mode="wrap"), conductance, source)
    potential = jnp.cumsum(tracer, axis=2) / GRID_Z
    return potential, tracer
```

```python
import functools

import jax
import jax.numpy as jnp
from jax import lax
from jax.experimental import pallas as pl
from jax.experimental.pallas import tpu as pltpu
from jax.sharding import PartitionSpec as P

MESH = pl.DeviceIdType.MESH
STEPS = 4
SLAB = 8
DOWN, UP = 0, 1


def kernel(
    rows, width, zsize, total_z,
    tracer, conductance, source,
    potential, end,
    even, odd, cond, src, z_out, z_in, p_out, p_in,
    load_sem, zs, zr, xs, xr, ys, yr, ps, pr,
):
    fields = (even, odd)
    axes = ("py", "px", "pz")
    me = {axis: lax.axis_index(axis) for axis in axes}
    near = {}
    for axis in axes:
        size = lax.axis_size(axis)
        near[axis] = (lax.rem(me[axis] + size - 1, size), lax.rem(me[axis] + 1, size))
    mz = me["pz"]
    last = rows - 1

    def row_at(i):
        half, odd_one = i // 2, i % 2
        return half + odd_one * (last - 2 * half)

    def load(which, y):
        if which == 0:
            place = even.at[1 + y, pl.ds(1, width)]
            return pltpu.make_async_copy(tracer.at[y], place, load_sem.at[0, y])
        array, place = ((conductance, cond), (source, src))[which - 1]
        return pltpu.make_async_copy(array.at[y], place.at[y], load_sem.at[which, y])

    def remote(a, b, send, recv, axis, way):
        return pltpu.make_async_remote_copy(
            src_ref=a, dst_ref=b, send_sem=send, recv_sem=recv,
            device_id={axis: near[axis][way]}, device_id_type=MESH,
        )

    def z_copy(par, way, y):
        return remote(
            z_out.at[par, way, y], z_in.at[par, way, y], zs.at[par, way, y], zr.at[par, way, y], "pz", way
        )

    def x_copy(par, way, y):
        field = fields[par]
        mine, theirs = ((1, width + 1), (width, 0))[way]
        return remote(
            field.at[1 + y, mine], field.at[1 + y, theirs], xs.at[par, way, y], xr.at[par, way, y], "px", way
        )

    def y_copy(par, way):
        field = fields[par]
        mine, theirs = ((1, rows + 1), (rows, 0))[way]
        inner = pl.ds(1, width)
        return remote(
            field.at[mine, inner], field.at[theirs, inner], ys.at[par, way], yr.at[par, way], "py", way
        )

    def p_copy(y):
        return remote(p_out.at[y], p_in.at[y], ps.at[y], pr.at[y], "pz", UP)

    def send_row(par, y):
        for way in (DOWN, UP):
            z_copy(par, way, y).start()
        for way in (DOWN, UP):
            x_copy(par, way, y).start()

        @pl.when(y == 0)
        def _():
            y_copy(par, DOWN).start()

        @pl.when(y == last)
        def _():
            y_copy(par, UP).start()

    def sent_row(par, y):
        for way in (DOWN, UP):
            z_copy(par, way, y).wait_send()
            x_copy(par, way, y).wait_send()

        @pl.when(y == 0)
        def _():
            y_copy(par, DOWN).wait_send()

        @pl.when(y == last)
        def _():
            y_copy(par, UP).wait_send()

    def arrived_row(par, y):
        for way in (DOWN, UP):
            x_copy(par, way, y).wait_recv()

        @pl.when(y == 0)
        def _():
            y_copy(par, UP).wait_recv()

        @pl.when(y == last)
        def _():
            y_copy(par, DOWN).wait_recv()

        for way in (DOWN, UP):
            z_copy(par, way, y).wait_recv()

    def each_row(body):
        def run(i, carry):
            body(row_at(i))
            return carry

        lax.fori_loop(0, rows, run, 0)

    def each_slab(body):
        def run(i, carry):
            body(pl.multiple_of(i * SLAB, SLAB))
            return carry

        lax.fori_loop(0, width // SLAB, run, 0)

    for which in (0, 1, 2):
        each_row(lambda y: load(which, y).start())

    barrier = pltpu.get_barrier_semaphore()
    for axis in axes:
        for way in (DOWN, UP):
            pl.semaphore_signal(barrier, inc=1, device_id={axis: near[axis][way]}, device_id_type=MESH)
    pl.semaphore_wait(barrier, 6)

    level = lax.broadcasted_iota(jnp.int32, (8, 128), 0)

    def first(y):
        load(0, y).wait()

        def slab(x0):
            for j in range(SLAB):
                value = even[1 + y, 1 + x0 + j]
                z_out[0, DOWN, y, pl.ds(x0 + j, 1), :] = value[0:1, :]
                z_out[0, UP, y, pl.ds(x0 + j, 1), :] = value[7:8, :]

        each_slab(slab)
        send_row(0, y)

    each_row(first)

    for step in range(1, STEPS + 1):
        old, new = (step - 1) % 2, step % 2
        before, after = fields[old], fields[new]

        def advance(y, step=step, old=old, new=new, before=before, after=after):
            if step == 1:
                load(1, y).wait()
                load(2, y).wait()
            if 2 <= step < STEPS:
                sent_row(new, y)
            arrived_row(old, y)

            def slab(x0):
                line = [before[1 + y, x0 + j] for j in range(SLAB + 2)]
                for j in range(SLAB):
                    x = x0 + j
                    here = line[j + 1]
                    low = z_in[old, UP, y, pl.ds(x, 1), :]
                    high = z_in[old, DOWN, y, pl.ds(x, 1), :]
                    around = (line[j] + line[j + 2]) + (before[y, 1 + x] + before[2 + y, 1 + x])
                    below = pltpu.roll(jnp.where(level == 7, low, here), 1, 0)
                    above = pltpu.roll(jnp.where(level == 0, high, here), 7, 0)
                    spread = around + (below + above) - 6.0 * here
                    value = here + cond[y, x] * spread + src[y, x]
                    if step < STEPS:
                        after[1 + y, 1 + x] = value
                        z_out[new, DOWN, y, pl.ds(x, 1), :] = value[0:1, :]
                        z_out[new, UP, y, pl.ds(x, 1), :] = value[7:8, :]
                    else:
                        end[y, x] = value
                        run = value
                        for shift in (1, 2, 4):
                            run = run + jnp.where(level >= shift, pltpu.roll(run, shift, 0), 0.0)
                        potential[y, x] = run
                        p_out[y, pl.ds(x, 1), :] = run[7:8, :]

            each_slab(slab)
            if step < STEPS:
                send_row(new, y)
            else:

                @pl.when(mz == 0)
                def _():
                    p_copy(y).start()

        each_row(advance)

    def finish(y):
        for par in (0, 1):
            sent_row(par, y)

        @pl.when(mz == 0)
        def _():
            p_in[y] = jnp.zeros_like(p_in[y])

        @pl.when(mz > 0)
        def _():
            p_copy(y).wait_recv()

            @pl.when(mz < zsize - 1)
            def _():
                p_out[y] += p_in[y]
                p_copy(y).start()

        def slab(x0):
            for j in range(SLAB):
                x = x0 + j
                potential[y, x] = (potential[y, x] + p_in[y, pl.ds(x, 1), :]) * (1.0 / total_z)

        each_slab(slab)

    each_row(finish)

    @pl.when(mz < zsize - 1)
    def _():
        each_row(lambda y: p_copy(y).wait_send())


def on_device(tracer, conductance, source):
    rows, width, depth, members = tracer.shape
    zsize = lax.axis_size("pz")
    block = (rows, width, depth, members)
    padded = (rows + 2, width + 2, depth, members)
    face = (rows, width, members)
    f32 = jnp.float32
    dma = pltpu.SemaphoreType.DMA
    cells = rows * width * depth * members
    return pl.pallas_call(
        functools.partial(kernel, rows, width, zsize, depth * zsize),
        out_shape=OUT(block),
        in_specs=[pl.BlockSpec(memory_space=pl.ANY)] * 3,
        out_specs=(pl.BlockSpec(memory_space=pltpu.VMEM),) * 2,
        scratch_shapes=[
            pltpu.VMEM(padded, f32),
            pltpu.VMEM(padded, f32),
            pltpu.VMEM(block, f32),
            pltpu.VMEM(block, f32),
            pltpu.VMEM((2, 2) + face, f32),
            pltpu.VMEM((2, 2) + face, f32),
            pltpu.VMEM(face, f32),
            pltpu.VMEM(face, f32),
            dma((3, rows)),
            dma((2, 2, rows)),
            dma((2, 2, rows)),
            dma((2, 2, rows)),
            dma((2, 2, rows)),
            dma((2, 2)),
            dma((2, 2)),
            dma((rows,)),
            dma((rows,)),
        ],
        compiler_params=pltpu.CompilerParams(
            collective_id=0, has_side_effects=True, vmem_limit_bytes=LIMIT
        ),
        cost_estimate=pl.CostEstimate(flops=48 * cells, bytes_accessed=20 * cells, transcendentals=0),
        name="diffuse",
    )(tracer, conductance, source)


LIMIT = 47 * 2**20


def OUT(block):
    return (pltpu.VMEM(block, jnp.float32), pltpu.VMEM(block, jnp.float32))


def solution(mesh):
    placed = P("py", "px", "pz", None)
    return jax.shard_map(
        on_device,
        mesh=mesh,
        in_specs=(placed, placed, placed),
        out_specs=(placed, placed),
        check_vma=False,
    )
```

```python
import functools

import jax
import jax.numpy as jnp
from jax import lax
from jax.experimental import pallas as pl
from jax.experimental.pallas import tpu as pltpu
from jax.sharding import PartitionSpec as P

MESH = pl.DeviceIdType.MESH
STEPS = 4
SLAB = 8
DOWN, UP = 0, 1

KINDS = ("chain", "low", "high", "middle")
ORIGINS = {
    "chain": ((UP, (0,)),),
    "low": ((UP, (1,)), (DOWN, (0,))),
    "high": ((UP, (0,)), (DOWN, (2,))),
    "middle": ((UP, (0, 2)), (DOWN, (1,))),
}
RELAYS = {
    "chain": ((UP, (1, 2), ()),),
    "low": ((UP, (2,), ()), (DOWN, (), (3, 2))),
    "high": ((UP, (1,), ()), (DOWN, (1, 0), ())),
    "middle": ((DOWN, (0,), (3,)),),
}


def kernel(
    rows, width, total_z,
    tracer, conductance, source,
    potential, end,
    even, odd, cond, src, z_out, z_in, total, p_in,
    load_sem, zs, zr, xs, xr, ys, yr, ps, pr,
):
    fields = (even, odd)
    axes = ("py", "px", "pz")
    me = {axis: lax.axis_index(axis) for axis in axes}
    near = {}
    for axis in axes:
        size = lax.axis_size(axis)
        near[axis] = (lax.rem(me[axis] + size - 1, size), lax.rem(me[axis] + 1, size))
    mz = me["pz"]
    last, quarter = rows - 1, rows // 4

    def row_at(i):
        half, odd_one = i // 2, i % 2
        return half + odd_one * (last - 2 * half)

    def load(which, y):
        if which == 0:
            place = even.at[1 + y, pl.ds(1, width)]
            return pltpu.make_async_copy(tracer.at[y], place, load_sem.at[0, y])
        array, place = ((conductance, cond), (source, src))[which - 1]
        return pltpu.make_async_copy(array.at[y], place.at[y], load_sem.at[which, y])

    def remote(a, b, send, recv, axis, way):
        return pltpu.make_async_remote_copy(
            src_ref=a, dst_ref=b, send_sem=send, recv_sem=recv,
            device_id={axis: near[axis][way]}, device_id_type=MESH,
        )

    def z_copy(par, way, y):
        return remote(
            z_out.at[par, way, y], z_in.at[par, way, y], zs.at[par, way, y], zr.at[par, way, y], "pz", way
        )

    def x_copy(par, way, y):
        field = fields[par]
        mine, theirs = ((1, width + 1), (width, 0))[way]
        return remote(
            field.at[1 + y, mine], field.at[1 + y, theirs], xs.at[par, way, y], xr.at[par, way, y], "px", way
        )

    def y_copy(par, way):
        field = fields[par]
        mine, theirs = ((1, rows + 1), (rows, 0))[way]
        inner = pl.ds(1, width)
        return remote(
            field.at[mine, inner], field.at[theirs, inner], ys.at[par, way], yr.at[par, way], "py", way
        )

    def p_copy(way, y, place):
        return remote(place, p_in.at[way, y], ps.at[way, y], pr.at[way, y], "pz", way)

    def p_arrived(way, y):
        p_copy(way, y, total.at[y]).wait_recv()

    def on(devices):
        hit = mz == devices[0]
        for device in devices[1:]:
            hit = jnp.logical_or(hit, mz == device)
        return pl.when(hit)

    def originate(kind, y):
        for way, devices in ORIGINS[kind]:

            @on(devices)
            def _():
                p_copy(way, y, total.at[y]).start()

    def relay(kind, way, device, y):
        adds = [pair[1] for pair in RELAYS[kind] if pair[0] == way][0]

        @on((device,))
        def _():
            p_arrived(way, y)
            if device in adds:
                z_in[0, way, y] = p_in[way, y] + total[y]
                p_copy(way, y, z_in.at[0, way, y]).start()
            else:
                p_copy(way, y, p_in.at[way, y]).start()

    def conclude(device, y, ways, waits=()):
        @on((device,))
        def _():
            for way in waits:
                p_arrived(way, y)

            def slab(x0):
                for j in range(SLAB):
                    x = x0 + j
                    below = p_in[ways[0], y, pl.ds(x, 1), :]
                    for way in ways[1:]:
                        below = below + p_in[way, y, pl.ds(x, 1), :]
                    potential[y, x] = potential[y, x] + below * (1.0 / total_z)

            each_slab(slab)

    def send_row(par, y):
        for way in (DOWN, UP):
            z_copy(par, way, y).start()
        for way in (DOWN, UP):
            x_copy(par, way, y).start()

        @pl.when(y == 0)
        def _():
            y_copy(par, DOWN).start()

        @pl.when(y == last)
        def _():
            y_copy(par, UP).start()

    def sent_row(par, y):
        for way in (DOWN, UP):
            z_copy(par, way, y).wait_send()
            x_copy(par, way, y).wait_send()

        @pl.when(y == 0)
        def _():
            y_copy(par, DOWN).wait_send()

        @pl.when(y == last)
        def _():
            y_copy(par, UP).wait_send()

    def arrived_row(par, y):
        for way in (DOWN, UP):
            x_copy(par, way, y).wait_recv()

        @pl.when(y == 0)
        def _():
            y_copy(par, UP).wait_recv()

        @pl.when(y == last)
        def _():
            y_copy(par, DOWN).wait_recv()

        for way in (DOWN, UP):
            z_copy(par, way, y).wait_recv()

    def each_row(body):
        def run(i, carry):
            body(row_at(i))
            return carry

        lax.fori_loop(0, rows, run, 0)

    def each_slab(body):
        def run(i, carry):
            body(pl.multiple_of(i * SLAB, SLAB))
            return carry

        lax.fori_loop(0, width // SLAB, run, 0)

    each_row(lambda y: load(0, y).start())

    barrier = pltpu.get_barrier_semaphore()
    for axis in axes:
        for way in (DOWN, UP):
            pl.semaphore_signal(barrier, inc=1, device_id={axis: near[axis][way]}, device_id_type=MESH)
    pl.semaphore_wait(barrier, 6)

    level = lax.broadcasted_iota(jnp.int32, (8, 128), 0)

    def first(y):
        load(0, y).wait()
        load(1, y).start()
        load(2, y).start()

        def slab(x0):
            for j in range(SLAB):
                value = even[1 + y, 1 + x0 + j]
                z_out[0, DOWN, y, pl.ds(x0 + j, 1), :] = value[0:1, :]
                z_out[0, UP, y, pl.ds(x0 + j, 1), :] = value[7:8, :]

        each_slab(slab)
        send_row(0, y)

    each_row(first)

    for step in range(1, STEPS + 1):
        old, new = (step - 1) % 2, step % 2
        before, after = fields[old], fields[new]

        def advance(y, step=step, old=old, new=new, before=before, after=after):
            if step == 1:
                load(1, y).wait()
                load(2, y).wait()
            if 2 <= step < STEPS:
                sent_row(new, y)
            arrived_row(old, y)

            def slab(x0):
                line = [before[1 + y, x0 + j] for j in range(SLAB + 2)]
                for j in range(SLAB):
                    x = x0 + j
                    here = line[j + 1]
                    low = z_in[old, UP, y, pl.ds(x, 1), :]
                    high = z_in[old, DOWN, y, pl.ds(x, 1), :]
                    around = (line[j] + line[j + 2]) + (before[y, 1 + x] + before[2 + y, 1 + x])
                    below = pltpu.roll(jnp.where(level == 7, low, here), 1, 0)
                    above = pltpu.roll(jnp.where(level == 0, high, here), 7, 0)
                    spread = around + (below + above) - 6.0 * here
                    value = here + cond[y, x] * spread + src[y, x]
                    if step < STEPS:
                        after[1 + y, 1 + x] = value
                        z_out[new, DOWN, y, pl.ds(x, 1), :] = value[0:1, :]
                        z_out[new, UP, y, pl.ds(x, 1), :] = value[7:8, :]
                    else:
                        end[y, x] = value
                        run = value
                        for shift in (1, 2, 4):
                            run = run + jnp.where(level >= shift, pltpu.roll(run, shift, 0), 0.0)
                        potential[y, x] = run * (1.0 / total_z)
                        total[y, pl.ds(x, 1), :] = run[7:8, :]

            each_slab(slab)
            if step < STEPS:
                send_row(new, y)

        if step < STEPS:
            each_row(advance)
            continue
        for place, kind in enumerate(KINDS):

            def run(k, carry, place=place, kind=kind):
                y = row_at(place * quarter + k)
                advance(y)
                originate(kind, y)
                return carry

            lax.fori_loop(0, quarter, run, 0)

    def each_quarter(body):
        def run(k, carry):
            body({kind: row_at(place * quarter + k) for place, kind in enumerate(KINDS)})
            return carry

        lax.fori_loop(0, quarter, run, 0)

    def first_hops(at):
        relay("chain", UP, 1, at["chain"])
        relay("high", DOWN, 1, at["high"])
        relay("low", UP, 2, at["low"])
        relay("low", DOWN, 3, at["low"])
        relay("middle", DOWN, 0, at["middle"])
        relay("low", DOWN, 2, at["low"])
        conclude(1, at["chain"], (UP,))
        conclude(2, at["low"], (UP, DOWN))

    def second_hops(at):
        relay("high", UP, 1, at["high"])
        relay("high", DOWN, 0, at["high"])
        relay("chain", UP, 2, at["chain"])
        relay("middle", DOWN, 3, at["middle"])
        for kind in KINDS:
            for par in (0, 1):
                sent_row(par, at[kind])
        conclude(1, at["high"], (UP,))
        conclude(2, at["chain"], (UP,))
        conclude(3, at["low"], (UP, DOWN), (UP,))
        conclude(3, at["middle"], (UP, DOWN), (UP,))

    def third_hops(at):
        conclude(1, at["low"], (DOWN,), (DOWN,))
        conclude(2, at["middle"], (DOWN,), (DOWN,))

    def last_hops(at):
        conclude(1, at["middle"], (UP,), (UP,))
        conclude(2, at["high"], (UP,), (UP,))
        conclude(3, at["chain"], (UP,), (UP,))
        conclude(3, at["high"], (DOWN,), (DOWN,))

    def all_sent(at):
        for kind in KINDS:
            for way in (DOWN, UP):
                devices = sum([pair[1] for pair in ORIGINS[kind] if pair[0] == way], ())
                devices += sum([pair[1] + pair[2] for pair in RELAYS[kind] if pair[0] == way], ())
                if devices:

                    @on(devices)
                    def _():
                        p_copy(way, at[kind], total.at[at[kind]]).wait_send()

    for body in (first_hops, second_hops, third_hops, last_hops, all_sent):
        each_quarter(body)


def on_device(tracer, conductance, source):
    rows, width, depth, members = tracer.shape
    zsize = lax.axis_size("pz")
    block = (rows, width, depth, members)
    padded = (rows + 2, width + 2, depth, members)
    face = (rows, width, members)
    f32 = jnp.float32
    dma = pltpu.SemaphoreType.DMA
    cells = rows * width * depth * members
    return pl.pallas_call(
        functools.partial(kernel, rows, width, depth * zsize),
        out_shape=(pltpu.VMEM(block, f32), pltpu.VMEM(block, f32)),
        in_specs=[pl.BlockSpec(memory_space=pl.ANY)] * 3,
        out_specs=(pl.BlockSpec(memory_space=pltpu.VMEM),) * 2,
        scratch_shapes=[
            pltpu.VMEM(padded, f32),
            pltpu.VMEM(padded, f32),
            pltpu.VMEM(block, f32),
            pltpu.VMEM(block, f32),
            pltpu.VMEM((2, 2) + face, f32),
            pltpu.VMEM((2, 2) + face, f32),
            pltpu.VMEM(face, f32),
            pltpu.VMEM((2,) + face, f32),
            dma((3, rows)),
            dma((2, 2, rows)),
            dma((2, 2, rows)),
            dma((2, 2, rows)),
            dma((2, 2, rows)),
            dma((2, 2)),
            dma((2, 2)),
            dma((2, rows)),
            dma((2, rows)),
        ],
        compiler_params=pltpu.CompilerParams(
            collective_id=0, has_side_effects=True, vmem_limit_bytes=47 * 2**20
        ),
        cost_estimate=pl.CostEstimate(flops=48 * cells, bytes_accessed=20 * cells, transcendentals=0),
        name="diffuse",
    )(tracer, conductance, source)


def solution(mesh):
    placed = P("py", "px", "pz", None)
    return jax.shard_map(
        on_device,
        mesh=mesh,
        in_specs=(placed, placed, placed),
        out_specs=(placed, placed),
        check_vma=False,
    )
```

```python
import functools

import jax
import jax.numpy as jnp
from jax import lax
from jax.experimental import pallas as pl
from jax.experimental.pallas import tpu as pltpu
from jax.sharding import PartitionSpec as P

MESH = pl.DeviceIdType.MESH
STEPS = 4
SLAB = 8
DOWN, UP = 0, 1

KINDS = ("chain", "low", "high", "middle")
ORIGINS = {
    "chain": ((UP, (0,)),),
    "low": ((UP, (1,)), (DOWN, (0,))),
    "high": ((UP, (0,)), (DOWN, (2,))),
    "middle": ((UP, (0, 2)), (DOWN, (1,))),
}
RELAYS = {
    "chain": ((UP, (1, 2), ()),),
    "low": ((UP, (2,), ()), (DOWN, (), (3, 2))),
    "high": ((UP, (1,), ()), (DOWN, (1, 0), ())),
    "middle": ((DOWN, (0,), (3,)),),
}

LAST = ((1, "middle", UP), (2, "high", UP), (3, "chain", UP), (3, "high", DOWN))


def row_of(rows, i):
    half, odd_one = i // 2, i % 2
    return half + odd_one * (rows - 1 - 2 * half)


def on(mz, devices):
    hit = mz == devices[0]
    for device in devices[1:]:
        hit = jnp.logical_or(hit, mz == device)
    return pl.when(hit)


def add_below(out, base, p_in, y, ways, scale):
    def run(i, carry):
        for j in range(SLAB):
            x = i * SLAB + j
            below = p_in[ways[0], y, pl.ds(x, 1), :]
            for way in ways[1:]:
                below = below + p_in[way, y, pl.ds(x, 1), :]
            out[x] = base[x] + below * scale
        return carry

    lax.fori_loop(0, base.shape[0] // SLAB, run, 0)


def kernel(
    rows, width, total_z,
    tracer, conductance, source,
    potential, end, p_in,
    even, odd, cond, src, z_out, z_in, total,
    load_sem, zs, zr, xs, xr, ys, yr, ps, pr,
):
    fields = (even, odd)
    axes = ("py", "px", "pz")
    me = {axis: lax.axis_index(axis) for axis in axes}
    near = {}
    for axis in axes:
        size = lax.axis_size(axis)
        near[axis] = (lax.rem(me[axis] + size - 1, size), lax.rem(me[axis] + 1, size))
    mz = me["pz"]
    last, quarter = rows - 1, rows // 4
    row_at = functools.partial(row_of, rows)

    def load_field(part):
        place = pl.ds(part * quarter, quarter)
        inside = even.at[pl.ds(1 + part * quarter, quarter), pl.ds(1, width)]
        return pltpu.make_async_copy(tracer.at[place], inside, load_sem.at[part])

    def load_rest():
        return (
            pltpu.make_async_copy(conductance, cond, load_sem.at[4]),
            pltpu.make_async_copy(source, src, load_sem.at[5]),
        )

    def remote(a, b, send, recv, axis, way):
        return pltpu.make_async_remote_copy(
            src_ref=a, dst_ref=b, send_sem=send, recv_sem=recv,
            device_id={axis: near[axis][way]}, device_id_type=MESH,
        )

    def z_copy(par, way, y):
        return remote(z_out.at[par, y, way], z_in.at[par, y, way], zs.at[par], zr.at[par, y], "pz", way)

    def z_all_sent(par):
        remote(z_out.at[par], z_in.at[par], zs.at[par], zr.at[par, 0], "pz", UP).wait_send()

    def z_arrived(par, y):
        remote(z_out.at[par, y], z_in.at[par, y], zs.at[par], zr.at[par, y], "pz", UP).wait_recv()

    def x_copy(par, way):
        field = fields[par]
        mine, theirs = ((1, width + 1), (width, 0))[way]
        inner = pl.ds(1, rows)
        return remote(
            field.at[inner, mine], field.at[inner, theirs], xs.at[par, way], xr.at[par, way], "px", way
        )

    def y_copy(par, way):
        field = fields[par]
        mine, theirs = ((1, rows + 1), (rows, 0))[way]
        inner = pl.ds(1, width)
        return remote(
            field.at[mine, inner], field.at[theirs, inner], ys.at[par, way], yr.at[par, way], "py", way
        )

    def p_copy(kind, way, y, place):
        return remote(place, p_in.at[way, y], ps.at[way, KINDS.index(kind)], pr.at[way, y], "pz", way)

    def p_arrived(way, y):
        p_copy(KINDS[0], way, y, total.at[y]).wait_recv()

    def p_all_sent(kind, way):
        group = pl.ds(0, quarter)
        sem = ps.at[way, KINDS.index(kind)]
        remote(total.at[group], p_in.at[way, group], sem, pr.at[way, 0], "pz", way).wait_send()

    def originate(kind, y):
        for way, devices in ORIGINS[kind]:

            @on(mz, devices)
            def _():
                p_copy(kind, way, y, total.at[y]).start()

    def relay(kind, way, device, y):
        adds = [pair[1] for pair in RELAYS[kind] if pair[0] == way][0]

        @on(mz, (device,))
        def _():
            p_arrived(way, y)
            if device in adds:
                z_in[0, y, way] = p_in[way, y] + total[y]
                p_copy(kind, way, y, z_in.at[0, y, way]).start()
            else:
                p_copy(kind, way, y, p_in.at[way, y]).start()

    def conclude(device, y, ways, waits=()):
        @on(mz, (device,))
        def _():
            for way in waits:
                p_arrived(way, y)

            add_below(potential.at[y], potential.at[y], p_in, y, ways, 1.0 / total_z)

    def send_row(par, y):
        for way in (DOWN, UP):
            z_copy(par, way, y).start()

        @pl.when(y == 0)
        def _():
            y_copy(par, DOWN).start()

        @pl.when(y == last)
        def _():
            y_copy(par, UP).start()

    def all_sent_of(par):
        z_all_sent(par)
        for way in (DOWN, UP):
            x_copy(par, way).wait_send()
            y_copy(par, way).wait_send()

    def arrived_row(par, y):
        @pl.when(y == 0)
        def _():
            y_copy(par, UP).wait_recv()

        @pl.when(y == last)
        def _():
            y_copy(par, DOWN).wait_recv()

        z_arrived(par, y)

    def each_row(body):
        def run(i, carry):
            body(row_at(i))
            return carry

        lax.fori_loop(0, rows, run, 0)

    def each_slab(body):
        def run(i, carry):
            body(pl.multiple_of(i * SLAB, SLAB))
            return carry

        lax.fori_loop(0, width // SLAB, run, 0)

    barrier = pltpu.get_barrier_semaphore()
    for axis in ("pz", "px", "py"):
        for way in (DOWN, UP):
            pl.semaphore_signal(barrier, inc=1, device_id={axis: near[axis][way]}, device_id_type=MESH)

    for part in (0, 3, 1, 2):
        load_field(part).start()

    level = lax.broadcasted_iota(jnp.int32, (8, 128), 0)

    def pack(y):
        def slab(x0):
            for j in range(SLAB):
                value = even[1 + y, 1 + x0 + j]
                z_out[0, y, DOWN, pl.ds(x0 + j, 1), :] = value[0:1, :]
                z_out[0, y, UP, pl.ds(x0 + j, 1), :] = value[7:8, :]

        each_slab(slab)

    def some_rows(low, high, body):
        lax.fori_loop(low, high, lambda i, carry: (body(row_at(i)), carry)[1], 0)

    def first(y):
        pack(y)
        send_row(0, y)

    for part in (0, 3):
        load_field(part).wait()
    for copy in load_rest():
        copy.start()
    some_rows(0, quarter, pack)
    pl.semaphore_wait(barrier, 6)
    some_rows(0, quarter, functools.partial(send_row, 0))
    some_rows(quarter, 2 * quarter, first)
    for part in (1, 2):
        load_field(part).wait()
    some_rows(2 * quarter, rows, first)
    for way in (DOWN, UP):
        x_copy(0, way).start()

    for step in range(1, STEPS + 1):
        old, new = (step - 1) % 2, step % 2
        before, after = fields[old], fields[new]
        if step == 1:
            for copy in load_rest():
                copy.wait()
        if 2 <= step < STEPS:
            all_sent_of(new)
        for way in (DOWN, UP):
            x_copy(old, way).wait_recv()

        def advance(y, step=step, old=old, new=new, before=before, after=after):
            arrived_row(old, y)

            def slab(x0):
                line = [before[1 + y, x0 + j] for j in range(SLAB + 2)]
                for j in range(SLAB):
                    x = x0 + j
                    here = line[j + 1]
                    low = z_in[old, y, UP, pl.ds(x, 1), :]
                    high = z_in[old, y, DOWN, pl.ds(x, 1), :]
                    around = (line[j] + line[j + 2]) + (before[y, 1 + x] + before[2 + y, 1 + x])
                    below = pltpu.roll(jnp.where(level == 7, low, here), 1, 0)
                    above = pltpu.roll(jnp.where(level == 0, high, here), 7, 0)
                    spread = around + (below + above) - 6.0 * here
                    value = here + cond[y, x] * spread + src[y, x]
                    if step < STEPS:
                        after[1 + y, 1 + x] = value
                        z_out[new, y, DOWN, pl.ds(x, 1), :] = value[0:1, :]
                        z_out[new, y, UP, pl.ds(x, 1), :] = value[7:8, :]
                    else:
                        end[y, x] = value
                        run = value
                        for shift in (1, 2, 4):
                            run = run + jnp.where(level >= shift, pltpu.roll(run, shift, 0), 0.0)
                        potential[y, x] = run * (1.0 / total_z)
                        total[y, pl.ds(x, 1), :] = run[7:8, :]

            each_slab(slab)
            if step < STEPS:
                send_row(new, y)

        if step < STEPS:
            each_row(advance)
            for way in (DOWN, UP):
                x_copy(new, way).start()
            continue
        for place, kind in enumerate(KINDS):

            def run(k, carry, place=place, kind=kind):
                y = row_at(place * quarter + k)
                advance(y)
                originate(kind, y)
                return carry

            lax.fori_loop(0, quarter, run, 0)

    def each_quarter(body):
        def run(k, carry):
            body({kind: row_at(place * quarter + k) for place, kind in enumerate(KINDS)})
            return carry

        lax.fori_loop(0, quarter, run, 0)

    def first_hops(at):
        relay("chain", UP, 1, at["chain"])
        relay("high", DOWN, 1, at["high"])
        relay("low", UP, 2, at["low"])
        relay("low", DOWN, 3, at["low"])
        relay("middle", DOWN, 0, at["middle"])
        relay("low", DOWN, 2, at["low"])
        conclude(1, at["chain"], (UP,))
        conclude(2, at["low"], (UP, DOWN))

    def second_hops(at):
        relay("high", UP, 1, at["high"])
        relay("high", DOWN, 0, at["high"])
        relay("chain", UP, 2, at["chain"])
        relay("middle", DOWN, 3, at["middle"])
        conclude(1, at["high"], (UP,))
        conclude(2, at["chain"], (UP,))
        conclude(3, at["low"], (UP, DOWN), (UP,))
        conclude(3, at["middle"], (UP, DOWN), (UP,))

    def third_hops(at):
        conclude(1, at["low"], (DOWN,), (DOWN,))
        conclude(2, at["middle"], (DOWN,), (DOWN,))

    def last_hops(at):
        for device, kind, way in LAST:

            @on(mz, (device,))
            def _():
                p_arrived(way, at[kind])

    each_quarter(first_hops)
    for par in (0, 1):
        all_sent_of(par)
    for body in (second_hops, third_hops, last_hops):
        each_quarter(body)
    for kind in KINDS:
        for way in (DOWN, UP):
            devices = sum([pair[1] for pair in ORIGINS[kind] if pair[0] == way], ())
            devices += sum([pair[1] + pair[2] for pair in RELAYS[kind] if pair[0] == way], ())
            if devices:

                @on(mz, devices)
                def _():
                    p_all_sent(kind, way)


def write_out(total_z, held, end, p_in, potential_out, end_out, added, sem):
    mz = lax.axis_index("pz")
    rows = end.shape[0]
    quarter = rows // 4

    def potential_copy(y, source):
        return pltpu.make_async_copy(source, potential_out.at[y], sem.at[1])

    end_copy = pltpu.make_async_copy(end, end_out, sem.at[0])
    end_copy.start()
    for place, kind in enumerate(KINDS):
        late = [(device, way) for device, other, way in LAST if other == kind]

        def run(k, carry, place=place, late=late):
            i = place * quarter + k
            y = row_of(rows, i)
            plain = mz >= 0
            for device, way in late:
                plain = jnp.logical_and(plain, mz != device)

                @on(mz, (device,))
                def _():
                    add_below(added.at[i], held.at[y], p_in, y, (way,), 1.0 / total_z)
                    potential_copy(y, added.at[i]).start()

            @pl.when(plain)
            def _():
                potential_copy(y, held.at[y]).start()

            return carry

        lax.fori_loop(0, quarter, run, 0)
    pltpu.make_async_copy(held, potential_out, sem.at[1]).wait()
    end_copy.wait()


def on_device(tracer, conductance, source):
    rows, width, depth, members = tracer.shape
    zsize = lax.axis_size("pz")
    block = (rows, width, depth, members)
    padded = (rows + 2, width + 2, depth, members)
    face = (rows, width, members)
    f32 = jnp.float32
    dma = pltpu.SemaphoreType.DMA
    cells = rows * width * depth * members
    held = pl.pallas_call(
        functools.partial(kernel, rows, width, depth * zsize),
        out_shape=(pltpu.VMEM(block, f32), pltpu.VMEM(block, f32), pltpu.VMEM((2,) + face, f32)),
        in_specs=[pl.BlockSpec(memory_space=pl.ANY)] * 3,
        out_specs=(pl.BlockSpec(memory_space=pltpu.VMEM),) * 3,
        scratch_shapes=[
            pltpu.VMEM(padded, f32),
            pltpu.VMEM(padded, f32),
            pltpu.VMEM(block, f32),
            pltpu.VMEM(block, f32),
            pltpu.VMEM((2, rows, 2, width, members), f32),
            pltpu.VMEM((2, rows, 2, width, members), f32),
            pltpu.VMEM(face, f32),
            dma((6,)),
            dma((2,)),
            dma((2, rows)),
            dma((2, 2)),
            dma((2, 2)),
            dma((2, 2)),
            dma((2, 2)),
            dma((2, len(KINDS))),
            dma((2, rows)),
        ],
        compiler_params=pltpu.CompilerParams(
            collective_id=0, has_side_effects=True, vmem_limit_bytes=45 * 2**20
        ),
        cost_estimate=pl.CostEstimate(flops=48 * cells, bytes_accessed=20 * cells, transcendentals=0),
        name="diffuse",
    )(tracer, conductance, source)
    return pl.pallas_call(
        functools.partial(write_out, depth * zsize),
        out_shape=(jax.ShapeDtypeStruct(block, f32),) * 2,
        in_specs=[pl.BlockSpec(memory_space=pltpu.VMEM)] * 3,
        out_specs=(pl.BlockSpec(memory_space=pl.ANY),) * 2,
        scratch_shapes=[pltpu.VMEM(block, f32), dma((2,))],
        compiler_params=pltpu.CompilerParams(vmem_limit_bytes=10 * 2**20),
        cost_estimate=pl.CostEstimate(flops=cells, bytes_accessed=8 * cells, transcendentals=0),
        name="write_out",
    )(*held)


def solution(mesh):
    placed = P("py", "px", "pz", None)
    return jax.shard_map(
        on_device,
        mesh=mesh,
        in_specs=(placed, placed, placed),
        out_specs=(placed, placed),
        check_vma=False,
    )
```

```python
import functools

import jax
import jax.numpy as jnp
from jax import lax
from jax.experimental import pallas as pl
from jax.experimental.pallas import tpu as pltpu
from jax.sharding import PartitionSpec as P

MESH = pl.DeviceIdType.MESH
STEPS = 4
SLAB = 8
DOWN, UP = 0, 1

KINDS = ("chain", "low", "high", "middle")
ORIGINS = {
    "chain": ((UP, (0,)),),
    "low": ((UP, (1,)), (DOWN, (0,))),
    "high": ((UP, (0,)), (DOWN, (2,))),
    "middle": ((UP, (0, 2)), (DOWN, (1,))),
}
RELAYS = {
    "chain": ((UP, (1, 2), ()),),
    "low": ((UP, (2,), ()), (DOWN, (), (3, 2))),
    "high": ((UP, (1,), ()), (DOWN, (1, 0), ())),
    "middle": ((DOWN, (0,), (3,)),),
}

LAST = ((1, "middle", UP), (2, "high", UP), (3, "chain", UP), (3, "high", DOWN))


def row_of(rows, i):
    half, odd_one = i // 2, i % 2
    return half + odd_one * (rows - 1 - 2 * half)


def on(mz, devices):
    hit = mz == devices[0]
    for device in devices[1:]:
        hit = jnp.logical_or(hit, mz == device)
    return pl.when(hit)


def add_below(out, base, p_in, y, ways, scale):
    def run(i, carry):
        for j in range(SLAB):
            x = i * SLAB + j
            below = p_in[ways[0], y, pl.ds(x, 1), :]
            for way in ways[1:]:
                below = below + p_in[way, y, pl.ds(x, 1), :]
            out[x] = base[x] + below * scale
        return carry

    lax.fori_loop(0, base.shape[0] // SLAB, run, 0)


def kernel(
    rows, width, total_z,
    tracer, conductance, source,
    potential, end, p_in,
    even, odd, cond, src, z_out, z_in, total,
    load_sem, zs, zr, xs, xr, ys, yr, ps, pr,
):
    fields = (even, odd)
    axes = ("py", "px", "pz")
    me = {axis: lax.axis_index(axis) for axis in axes}
    near = {}
    for axis in axes:
        size = lax.axis_size(axis)
        near[axis] = (lax.rem(me[axis] + size - 1, size), lax.rem(me[axis] + 1, size))
    mz = me["pz"]
    last, quarter = rows - 1, rows // 4
    row_at = functools.partial(row_of, rows)

    parts = (((0, 1), (last, 1)), ((1, quarter - 1), (last - quarter + 1, quarter - 1)), ((quarter, 2 * quarter),))

    def rows_copy(start, size, sem):
        inside = even.at[pl.ds(1 + start, size), pl.ds(1, width)]
        return pltpu.make_async_copy(tracer.at[pl.ds(start, size)], inside, sem)

    def start_part(part):
        for start, size in parts[part]:
            rows_copy(start, size, load_sem.at[part]).start()

    def wait_part(part):
        rows_copy(0, sum(size for _, size in parts[part]), load_sem.at[part]).wait()

    def load_rest():
        return (
            pltpu.make_async_copy(conductance, cond, load_sem.at[3]),
            pltpu.make_async_copy(source, src, load_sem.at[4]),
        )

    def remote(a, b, send, recv, axis, way):
        return pltpu.make_async_remote_copy(
            src_ref=a, dst_ref=b, send_sem=send, recv_sem=recv,
            device_id={axis: near[axis][way]}, device_id_type=MESH,
        )

    def z_sem(par, y):
        index = turn_of(y)
        return zr.at[index // quarter] if par == 0 else zr.at[4 + index]

    def turn_of(y):
        far = y // (rows // 2)
        return 2 * (y + far * (last - 2 * y)) + far

    def z_copy(par, way, y):
        return remote(z_out.at[par, y, way], z_in.at[par, y, way], zs.at[par], z_sem(par, y), "pz", way)

    def z_all_sent(par):
        remote(z_out.at[par], z_in.at[par], zs.at[par], zr.at[0], "pz", UP).wait_send()

    def z_arrived(par, y):
        if par == 1:
            remote(z_out.at[par, y], z_in.at[par, y], zs.at[par], z_sem(par, y), "pz", UP).wait_recv()
            return
        group = pl.ds(0, quarter)

        @pl.when(turn_of(y) % quarter == 0)
        def _():
            remote(z_out.at[par, group], z_in.at[par, group], zs.at[par], z_sem(par, y), "pz", UP).wait_recv()

    def x_copy(par, way):
        field = fields[par]
        mine, theirs = ((1, width + 1), (width, 0))[way]
        inner = pl.ds(1, rows)
        return remote(field.at[inner, mine], field.at[inner, theirs], xs.at[par], xr.at[par], "px", way)

    def x_both(par):
        place = fields[par].at[pl.ds(1, rows), pl.ds(0, 2)]
        return remote(place, place, xs.at[par], xr.at[par], "px", UP)

    def y_copy(par, way):
        field = fields[par]
        mine, theirs = ((1, rows + 1), (rows, 0))[way]
        inner = pl.ds(1, width)
        return remote(field.at[mine, inner], field.at[theirs, inner], ys.at[par], yr.at[par], "py", way)

    def y_both(par):
        place = fields[par].at[pl.ds(0, 2), pl.ds(1, width)]
        return remote(place, place, ys.at[par], yr.at[par], "py", UP)

    def p_copy(kind, way, y, place):
        return remote(place, p_in.at[way, y], ps.at[way], pr.at[way, y], "pz", way)

    def p_arrived(way, y):
        p_copy(KINDS[0], way, y, total.at[y]).wait_recv()

    def p_all_sent(way, device):
        count = sum(
            quarter
            for kind in KINDS
            for other, *groups in ORIGINS[kind] + RELAYS[kind]
            if other == way and device in sum(groups, ())
        )
        if count:

            @on(mz, (device,))
            def _():
                group = pl.ds(0, count)
                remote(total.at[group], p_in.at[way, group], ps.at[way], pr.at[way, 0], "pz", way).wait_send()

    def originate(kind, y):
        for way, devices in ORIGINS[kind]:

            @on(mz, devices)
            def _():
                p_copy(kind, way, y, total.at[y]).start()

    def relay(kind, way, device, y):
        adds = [pair[1] for pair in RELAYS[kind] if pair[0] == way][0]

        @on(mz, (device,))
        def _():
            p_arrived(way, y)
            if device in adds:
                z_in[0, y, way] = p_in[way, y] + total[y]
                p_copy(kind, way, y, z_in.at[0, y, way]).start()
            else:
                p_copy(kind, way, y, p_in.at[way, y]).start()

    def conclude(device, y, ways, waits=()):
        @on(mz, (device,))
        def _():
            for way in waits:
                p_arrived(way, y)

            add_below(potential.at[y], potential.at[y], p_in, y, ways, 1.0 / total_z)

    def send_row(par, y):
        for way in (DOWN, UP):
            z_copy(par, way, y).start()

        @pl.when(y == 0)
        def _():
            y_copy(par, DOWN).start()

        @pl.when(y == last)
        def _():
            y_copy(par, UP).start()

    def all_sent_of(par):
        z_all_sent(par)
        x_both(par).wait_send()
        y_both(par).wait_send()

    def arrived_row(par, y):
        @pl.when(y == 0)
        def _():
            y_both(par).wait_recv()

        z_arrived(par, y)

    def each_row(body):
        def run(i, carry):
            body(row_at(i))
            return carry

        lax.fori_loop(0, rows, run, 0)

    def each_slab(body):
        def run(i, carry):
            body(pl.multiple_of(i * SLAB, SLAB))
            return carry

        lax.fori_loop(0, width // SLAB, run, 0)

    barrier = pltpu.get_barrier_semaphore()
    for axis in ("pz", "px", "py"):
        for way in (DOWN, UP):
            pl.semaphore_signal(barrier, inc=1, device_id={axis: near[axis][way]}, device_id_type=MESH)

    for part in range(len(parts)):
        start_part(part)

    level = lax.broadcasted_iota(jnp.int32, (8, 128), 0)

    def pack(y):
        def slab(x0):
            for j in range(SLAB):
                value = even[1 + y, 1 + x0 + j]
                z_out[0, y, DOWN, pl.ds(x0 + j, 1), :] = value[0:1, :]
                z_out[0, y, UP, pl.ds(x0 + j, 1), :] = value[7:8, :]

        each_slab(slab)

    def some_rows(low, high, body):
        lax.fori_loop(low, high, lambda i, carry: (body(row_at(i)), carry)[1], 0)

    def first(y):
        pack(y)
        send_row(0, y)

    wait_part(0)
    some_rows(0, 2, pack)
    pl.semaphore_wait(barrier, 6)
    some_rows(0, 2, functools.partial(send_row, 0))
    wait_part(1)
    some_rows(2, 2 * quarter, first)
    wait_part(2)
    for copy in load_rest():
        copy.start()
    some_rows(2 * quarter, rows, first)
    for way in (DOWN, UP):
        x_copy(0, way).start()

    for step in range(1, STEPS + 1):
        old, new = (step - 1) % 2, step % 2
        before, after = fields[old], fields[new]
        if step == 1:
            for copy in load_rest():
                copy.wait()
        if 2 <= step < STEPS:
            all_sent_of(new)
        x_both(old).wait_recv()

        def advance(y, step=step, old=old, new=new, before=before, after=after):
            arrived_row(old, y)

            def slab(x0):
                line = [before[1 + y, x0 + j] for j in range(SLAB + 2)]
                for j in range(SLAB):
                    x = x0 + j
                    here = line[j + 1]
                    low = z_in[old, y, UP, pl.ds(x, 1), :]
                    high = z_in[old, y, DOWN, pl.ds(x, 1), :]
                    around = (line[j] + line[j + 2]) + (before[y, 1 + x] + before[2 + y, 1 + x])
                    below = pltpu.roll(jnp.where(level == 7, low, here), 1, 0)
                    above = pltpu.roll(jnp.where(level == 0, high, here), 7, 0)
                    spread = around + (below + above) - 6.0 * here
                    value = here + cond[y, x] * spread + src[y, x]
                    if step < STEPS:
                        after[1 + y, 1 + x] = value
                        z_out[new, y, DOWN, pl.ds(x, 1), :] = value[0:1, :]
                        z_out[new, y, UP, pl.ds(x, 1), :] = value[7:8, :]
                    else:
                        end[y, x] = value
                        run = value
                        for shift in (1, 2, 4):
                            run = run + jnp.where(level >= shift, pltpu.roll(run, shift, 0), 0.0)
                        potential[y, x] = run * (1.0 / total_z)
                        total[y, pl.ds(x, 1), :] = run[7:8, :]

            each_slab(slab)
            if step < STEPS:
                send_row(new, y)

        if step < STEPS:
            each_row(advance)
            for way in (DOWN, UP):
                x_copy(new, way).start()
            continue
        for place, kind in enumerate(KINDS):

            def run(k, carry, place=place, kind=kind):
                y = row_at(place * quarter + k)
                advance(y)
                originate(kind, y)
                return carry

            lax.fori_loop(0, quarter, run, 0)

    def each_quarter(body):
        def run(k, carry):
            body({kind: row_at(place * quarter + k) for place, kind in enumerate(KINDS)})
            return carry

        lax.fori_loop(0, quarter, run, 0)

    def first_hops(at):
        relay("chain", UP, 1, at["chain"])
        relay("high", DOWN, 1, at["high"])
        relay("low", UP, 2, at["low"])
        relay("low", DOWN, 3, at["low"])
        relay("middle", DOWN, 0, at["middle"])
        relay("low", DOWN, 2, at["low"])
        conclude(1, at["chain"], (UP,))
        conclude(2, at["low"], (UP, DOWN))

    def second_hops(at):
        relay("high", UP, 1, at["high"])
        relay("high", DOWN, 0, at["high"])
        relay("chain", UP, 2, at["chain"])
        relay("middle", DOWN, 3, at["middle"])
        conclude(1, at["high"], (UP,))
        conclude(2, at["chain"], (UP,))
        conclude(3, at["low"], (UP, DOWN), (UP,))
        conclude(3, at["middle"], (UP, DOWN), (UP,))

    def third_hops(at):
        conclude(1, at["low"], (DOWN,), (DOWN,))
        conclude(2, at["middle"], (DOWN,), (DOWN,))

    def last_hops(at):
        for device, kind, way in LAST:

            @on(mz, (device,))
            def _():
                p_arrived(way, at[kind])

    each_quarter(first_hops)
    for par in (0, 1):
        all_sent_of(par)
    for body in (second_hops, third_hops, last_hops):
        each_quarter(body)
    for device in range(4):
        for way in (DOWN, UP):
            p_all_sent(way, device)


def write_out(total_z, held, end, p_in, potential_out, end_out, added, sem):
    mz = lax.axis_index("pz")
    rows = end.shape[0]
    quarter = rows // 4

    def potential_copy(y, source):
        return pltpu.make_async_copy(source, potential_out.at[y], sem.at[1])

    end_copy = pltpu.make_async_copy(end, end_out, sem.at[0])
    for place in range(4):
        part = pl.ds(place * quarter, quarter)
        pltpu.make_async_copy(end.at[part], end_out.at[part], sem.at[0]).start()
    for place, kind in enumerate(KINDS):
        late = [(device, way) for device, other, way in LAST if other == kind]

        def run(k, carry, place=place, late=late):
            i = place * quarter + k
            y = row_of(rows, i)
            plain = mz >= 0
            for device, way in late:
                plain = jnp.logical_and(plain, mz != device)

                @on(mz, (device,))
                def _():
                    add_below(added.at[i], held.at[y], p_in, y, (way,), 1.0 / total_z)
                    potential_copy(y, added.at[i]).start()

            @pl.when(plain)
            def _():
                potential_copy(y, held.at[y]).start()

            return carry

        lax.fori_loop(0, quarter, run, 0)
    pltpu.make_async_copy(held, potential_out, sem.at[1]).wait()
    end_copy.wait()


def on_device(tracer, conductance, source):
    rows, width, depth, members = tracer.shape
    zsize = lax.axis_size("pz")
    block = (rows, width, depth, members)
    padded = (rows + 2, width + 2, depth, members)
    face = (rows, width, members)
    f32 = jnp.float32
    dma = pltpu.SemaphoreType.DMA
    cells = rows * width * depth * members
    held = pl.pallas_call(
        functools.partial(kernel, rows, width, depth * zsize),
        out_shape=(pltpu.VMEM(block, f32), pltpu.VMEM(block, f32), pltpu.VMEM((2,) + face, f32)),
        in_specs=[pl.BlockSpec(memory_space=pl.ANY)] * 3,
        out_specs=(pl.BlockSpec(memory_space=pltpu.VMEM),) * 3,
        scratch_shapes=[
            pltpu.VMEM(padded, f32),
            pltpu.VMEM(padded, f32),
            pltpu.VMEM(block, f32),
            pltpu.VMEM(block, f32),
            pltpu.VMEM((2, rows, 2, width, members), f32),
            pltpu.VMEM((2, rows, 2, width, members), f32),
            pltpu.VMEM(face, f32),
            dma((5,)),
            dma((2,)),
            dma((4 + rows,)),
            dma((2,)),
            dma((2,)),
            dma((2,)),
            dma((2,)),
            dma((2,)),
            dma((2, rows)),
        ],
        compiler_params=pltpu.CompilerParams(
            collective_id=0, has_side_effects=True, vmem_limit_bytes=45 * 2**20
        ),
        cost_estimate=pl.CostEstimate(flops=48 * cells, bytes_accessed=20 * cells, transcendentals=0),
        name="diffuse",
    )(tracer, conductance, source)
    return pl.pallas_call(
        functools.partial(write_out, depth * zsize),
        out_shape=(jax.ShapeDtypeStruct(block, f32),) * 2,
        in_specs=[pl.BlockSpec(memory_space=pltpu.VMEM)] * 3,
        out_specs=(pl.BlockSpec(memory_space=pl.ANY),) * 2,
        scratch_shapes=[pltpu.VMEM(block, f32), dma((2,))],
        compiler_params=pltpu.CompilerParams(vmem_limit_bytes=10 * 2**20),
        cost_estimate=pl.CostEstimate(flops=cells, bytes_accessed=8 * cells, transcendentals=0),
        name="write_out",
    )(*held)


def solution(mesh):
    placed = P("py", "px", "pz", None)
    return jax.shard_map(
        on_device,
        mesh=mesh,
        in_specs=(placed, placed, placed),
        out_specs=(placed, placed),
        check_vma=False,
    )
```

```python
import functools

import jax
import jax.numpy as jnp
from jax import lax
from jax.experimental import pallas as pl
from jax.experimental.pallas import tpu as pltpu
from jax.sharding import PartitionSpec as P

MESH = pl.DeviceIdType.MESH
STEPS = 4
SLAB = 8
DOWN, UP = 0, 1

SHARES = {"chain": 5, "two": 2, "one": 2, "low": 3, "high": 3, "middle": 1}
ORIGINS = {
    "chain": ((UP, (0,)),),
    "two": ((DOWN, (2,)),),
    "one": ((DOWN, (1,)), (UP, (2,))),
    "low": ((UP, (1,)), (DOWN, (0,))),
    "high": ((UP, (0,)), (DOWN, (2,))),
    "middle": ((UP, (0, 2)), (DOWN, (1,))),
}
LATE_ORIGINS = {"two": ((UP, (0,)),)}
RELAYS = {
    "chain": ((UP, (1, 2), ()),),
    "two": ((DOWN, (1, 0), (3,)),),
    "one": ((DOWN, (0,), (3, 2)),),
    "low": ((UP, (2,), ()), (DOWN, (), (3, 2))),
    "high": ((UP, (1,), ()), (DOWN, (1, 0), ())),
    "middle": ((DOWN, (0,), (3,)),),
}
LAST = {
    (1, "one"): (DOWN, True),
    (1, "middle"): (UP, False),
    (1, "two"): (UP, False),
    (2, "high"): (UP, False),
    (2, "two"): (DOWN, True),
    (3, "chain"): (UP, False),
    (3, "high"): (DOWN, False),
}


def groups_of(rows):
    start, groups = 0, {}
    for kind, share in SHARES.items():
        groups[kind] = (start, start + share * rows // 16)
        start = groups[kind][1]
    return groups


def row_of(rows, i):
    half, odd_one = i // 2, i % 2
    return half + odd_one * (rows - 1 - 2 * half)


def on(mz, devices):
    hit = mz == devices[0]
    for device in devices[1:]:
        hit = jnp.logical_or(hit, mz == device)
    return pl.when(hit)


def add_below(out, base, p_in, y, ways, scale, own=None):
    def run(i, carry):
        for j in range(SLAB):
            x = i * SLAB + j
            below = p_in[ways[0], y, pl.ds(x, 1), :]
            for way in ways[1:]:
                below = below + p_in[way, y, pl.ds(x, 1), :]
            if own is not None:
                below = below - own[y, pl.ds(x, 1), :]
            out[x] = base[x] + below * scale
        return carry

    lax.fori_loop(0, base.shape[0] // SLAB, run, 0)


def kernel(
    rows, width, total_z,
    tracer, conductance, source,
    potential, end, p_in, total,
    even, odd, cond, src, z_out, z_in,
    load_sem, zs, zr, xs, xr, ys, yr, ps, pr,
):
    fields = (even, odd)
    axes = ("py", "px", "pz")
    me = {axis: lax.axis_index(axis) for axis in axes}
    near = {}
    for axis in axes:
        size = lax.axis_size(axis)
        near[axis] = (lax.rem(me[axis] + size - 1, size), lax.rem(me[axis] + 1, size))
    mz = me["pz"]
    last, quarter = rows - 1, rows // 4
    row_at = functools.partial(row_of, rows)

    parts = (((0, 1), (last, 1)), ((1, quarter - 1), (last - quarter + 1, quarter - 1)), ((quarter, 2 * quarter),))

    def rows_copy(start, size, sem):
        inside = even.at[pl.ds(1 + start, size), pl.ds(1, width)]
        return pltpu.make_async_copy(tracer.at[pl.ds(start, size)], inside, sem)

    def start_part(part):
        for start, size in parts[part]:
            rows_copy(start, size, load_sem.at[part]).start()

    def wait_part(part):
        rows_copy(0, sum(size for _, size in parts[part]), load_sem.at[part]).wait()

    def load_rest():
        return (
            pltpu.make_async_copy(conductance, cond, load_sem.at[3]),
            pltpu.make_async_copy(source, src, load_sem.at[4]),
        )

    def remote(a, b, send, recv, axis, way):
        return pltpu.make_async_remote_copy(
            src_ref=a, dst_ref=b, send_sem=send, recv_sem=recv,
            device_id={axis: near[axis][way]}, device_id_type=MESH,
        )

    def z_sem(par, y):
        index = turn_of(y)
        return zr.at[index // quarter] if par == 0 else zr.at[4 + index]

    def turn_of(y):
        far = y // (rows // 2)
        return 2 * (y + far * (last - 2 * y)) + far

    def z_copy(par, way, y):
        return remote(z_out.at[par, y, way], z_in.at[par, y, way], zs.at[par], z_sem(par, y), "pz", way)

    def z_all_sent(par):
        remote(z_out.at[par], z_in.at[par], zs.at[par], zr.at[0], "pz", UP).wait_send()

    def z_arrived(par, y):
        if par == 1:
            remote(z_out.at[par, y], z_in.at[par, y], zs.at[par], z_sem(par, y), "pz", UP).wait_recv()
            return
        group = pl.ds(0, quarter)

        @pl.when(turn_of(y) % quarter == 0)
        def _():
            remote(z_out.at[par, group], z_in.at[par, group], zs.at[par], z_sem(par, y), "pz", UP).wait_recv()

    def x_copy(par, way):
        field = fields[par]
        mine, theirs = ((1, width + 1), (width, 0))[way]
        inner = pl.ds(1, rows)
        return remote(field.at[inner, mine], field.at[inner, theirs], xs.at[par], xr.at[par], "px", way)

    def x_both(par):
        place = fields[par].at[pl.ds(1, rows), pl.ds(0, 2)]
        return remote(place, place, xs.at[par], xr.at[par], "px", UP)

    def y_copy(par, way):
        field = fields[par]
        mine, theirs = ((1, rows + 1), (rows, 0))[way]
        inner = pl.ds(1, width)
        return remote(field.at[mine, inner], field.at[theirs, inner], ys.at[par], yr.at[par], "py", way)

    def y_both(par):
        place = fields[par].at[pl.ds(0, 2), pl.ds(1, width)]
        return remote(place, place, ys.at[par], yr.at[par], "py", UP)

    def p_copy(way, y, place):
        return remote(place, p_in.at[way, y], ps.at[way], pr.at[way, y], "pz", way)

    def p_arrived(way, y):
        p_copy(way, y, total.at[y]).wait_recv()

    groups = groups_of(rows)

    def p_all_sent(way, device):
        count = sum(
            groups[kind][1] - groups[kind][0]
            for kind in SHARES
            for other, *devices in ORIGINS[kind] + LATE_ORIGINS.get(kind, ()) + RELAYS[kind]
            if other == way and device in sum(devices, ())
        )
        if count:

            @on(mz, (device,))
            def _():
                group = pl.ds(0, count)
                remote(total.at[group], p_in.at[way, group], ps.at[way], pr.at[way, 0], "pz", way).wait_send()

    def originate(origins, y):
        for way, devices in origins:

            @on(mz, devices)
            def _():
                p_copy(way, y, total.at[y]).start()

    def relay(kind, way, device, k):
        y = row_at(groups[kind][0] + k)
        adds = [pair[1] for pair in RELAYS[kind] if pair[0] == way][0]
        p_arrived(way, y)
        if device in adds:
            z_in[0, y, way] = p_in[way, y] + total[y]
            p_copy(way, y, z_in.at[0, y, way]).start()
        else:
            p_copy(way, y, p_in.at[way, y]).start()

    def conclude(kind, k, ways, waits=()):
        y = row_at(groups[kind][0] + k)
        for way in waits:
            p_arrived(way, y)
        add_below(potential.at[y], potential.at[y], p_in, y, ways, 1.0 / total_z)

    def send_row(par, y):
        for way in (DOWN, UP):
            z_copy(par, way, y).start()

        @pl.when(y == 0)
        def _():
            y_copy(par, DOWN).start()

        @pl.when(y == last)
        def _():
            y_copy(par, UP).start()

    def all_sent_of(par):
        z_all_sent(par)
        x_both(par).wait_send()
        y_both(par).wait_send()

    def arrived_row(par, y):
        @pl.when(y == 0)
        def _():
            y_both(par).wait_recv()

        z_arrived(par, y)

    def each_row(body):
        def run(i, carry):
            body(row_at(i))
            return carry

        lax.fori_loop(0, rows, run, 0)

    def each_slab(body):
        def run(i, carry):
            body(pl.multiple_of(i * SLAB, SLAB))
            return carry

        lax.fori_loop(0, width // SLAB, run, 0)

    barrier = pltpu.get_barrier_semaphore()
    for axis in ("pz", "px", "py"):
        for way in (DOWN, UP):
            pl.semaphore_signal(barrier, inc=1, device_id={axis: near[axis][way]}, device_id_type=MESH)

    for part in range(len(parts)):
        start_part(part)

    level = lax.broadcasted_iota(jnp.int32, (8, 128), 0)

    def pack(y):
        def slab(x0):
            for j in range(SLAB):
                value = even[1 + y, 1 + x0 + j]
                z_out[0, y, DOWN, pl.ds(x0 + j, 1), :] = value[0:1, :]
                z_out[0, y, UP, pl.ds(x0 + j, 1), :] = value[7:8, :]

        each_slab(slab)

    def some_rows(low, high, body):
        lax.fori_loop(low, high, lambda i, carry: (body(row_at(i)), carry)[1], 0)

    def first(y):
        pack(y)
        send_row(0, y)

    wait_part(0)
    some_rows(0, 2, pack)
    pl.semaphore_wait(barrier, 6)
    some_rows(0, 2, functools.partial(send_row, 0))
    wait_part(1)
    some_rows(2, 2 * quarter, first)
    wait_part(2)
    for copy in load_rest():
        copy.start()
    some_rows(2 * quarter, rows, first)
    for way in (DOWN, UP):
        x_copy(0, way).start()

    for step in range(1, STEPS + 1):
        old, new = (step - 1) % 2, step % 2
        before, after = fields[old], fields[new]
        if step == 1:
            for copy in load_rest():
                copy.wait()
        if 2 <= step < STEPS:
            all_sent_of(new)
        x_both(old).wait_recv()

        def advance(y, step=step, old=old, new=new, before=before, after=after):
            arrived_row(old, y)

            def slab(x0):
                line = [before[1 + y, x0 + j] for j in range(SLAB + 2)]
                for j in range(SLAB):
                    x = x0 + j
                    here = line[j + 1]
                    low = z_in[old, y, UP, pl.ds(x, 1), :]
                    high = z_in[old, y, DOWN, pl.ds(x, 1), :]
                    around = (line[j] + line[j + 2]) + (before[y, 1 + x] + before[2 + y, 1 + x])
                    below = pltpu.roll(jnp.where(level == 7, low, here), 1, 0)
                    above = pltpu.roll(jnp.where(level == 0, high, here), 7, 0)
                    spread = around + (below + above) - 6.0 * here
                    value = here + cond[y, x] * spread + src[y, x]
                    if step < STEPS:
                        after[1 + y, 1 + x] = value
                        z_out[new, y, DOWN, pl.ds(x, 1), :] = value[0:1, :]
                        z_out[new, y, UP, pl.ds(x, 1), :] = value[7:8, :]
                    else:
                        end[y, x] = value
                        run = value
                        for shift in (1, 2, 4):
                            run = run + jnp.where(level >= shift, pltpu.roll(run, shift, 0), 0.0)
                        potential[y, x] = run * (1.0 / total_z)
                        total[y, pl.ds(x, 1), :] = run[7:8, :]

            each_slab(slab)
            if step < STEPS:
                send_row(new, y)

        if step < STEPS:
            each_row(advance)
            for way in (DOWN, UP):
                x_copy(new, way).start()
            continue
        for kind, (low, high) in groups.items():

            def last_step(i, carry, kind=kind):
                y = row_at(i)
                advance(y)
                originate(ORIGINS[kind], y)
                return carry

            lax.fori_loop(low, high, last_step, 0)
        for kind, origins in LATE_ORIGINS.items():
            for i in range(*groups[kind]):
                originate(origins, row_at(i))

    def each(kind):
        return range(groups[kind][1] - groups[kind][0])

    @on(mz, (0,))
    def _():
        for kind in ("one", "middle", "two", "high"):
            for k in each(kind):
                relay(kind, DOWN, 0, k)

    @on(mz, (1,))
    def _():
        downs = [(kind, k) for kind in ("two", "high") for k in each(kind)]
        for k in each("chain"):
            relay("chain", UP, 1, k)
            if k < len(downs):
                relay(downs[k][0], DOWN, 1, downs[k][1])
        for k in each("chain"):
            conclude("chain", k, (UP,))
        for k in each("high"):
            relay("high", UP, 1, k)
            conclude("high", k, (UP,))
        for k in each("low"):
            conclude("low", k, (DOWN,), (DOWN,))

    @on(mz, (2,))
    def _():
        for k in each("low"):
            relay("low", UP, 2, k)
        downs = [(kind, k) for kind in ("low", "one") for k in each(kind)]
        for k in each("chain"):
            if k < len(downs):
                relay(downs[k][0], DOWN, 2, downs[k][1])
            relay("chain", UP, 2, k)
        for k in each("low"):
            conclude("low", k, (UP, DOWN))
        for k in each("chain"):
            conclude("chain", k, (UP,))
        for k in each("one"):
            conclude("one", k, (DOWN,))
        for k in each("middle"):
            conclude("middle", k, (DOWN,), (DOWN,))

    @on(mz, (3,))
    def _():
        for kind in ("low", "one", "middle", "two"):
            for k in each(kind):
                relay(kind, DOWN, 3, k)
        for kind in ("one", "middle", "low"):
            for k in each(kind):
                conclude(kind, k, (UP, DOWN), (UP,))
        for k in each("two"):
            conclude("two", k, (DOWN,))

    for (device, kind), (way, _) in LAST.items():

        @on(mz, (device,))
        def _():
            for i in range(*groups[kind]):
                p_arrived(way, row_at(i))

    for par in (0, 1):
        all_sent_of(par)
    for device in range(4):
        for way in (DOWN, UP):
            p_all_sent(way, device)


def write_out(total_z, held, end, p_in, total, potential_out, end_out, added, sem):
    mz = lax.axis_index("pz")
    rows = end.shape[0]
    quarter = rows // 4

    def potential_copy(y, source):
        return pltpu.make_async_copy(source, potential_out.at[y], sem.at[1])

    end_copy = pltpu.make_async_copy(end, end_out, sem.at[0])
    for place in range(4):
        part = pl.ds(place * quarter, quarter)
        pltpu.make_async_copy(end.at[part], end_out.at[part], sem.at[0]).start()
    for kind, (low, high) in groups_of(rows).items():
        late = [(device, *how) for (device, other), how in LAST.items() if other == kind]

        def run(i, carry, late=late):
            y = row_of(rows, i)
            plain = mz >= 0
            for device, way, off in late:
                plain = jnp.logical_and(plain, mz != device)

                @on(mz, (device,))
                def _():
                    own = total if off else None
                    add_below(added.at[i], held.at[y], p_in, y, (way,), 1.0 / total_z, own)
                    potential_copy(y, added.at[i]).start()

            @pl.when(plain)
            def _():
                potential_copy(y, held.at[y]).start()

            return carry

        lax.fori_loop(low, high, run, 0)
    pltpu.make_async_copy(held, potential_out, sem.at[1]).wait()
    end_copy.wait()


def on_device(tracer, conductance, source):
    rows, width, depth, members = tracer.shape
    zsize = lax.axis_size("pz")
    block = (rows, width, depth, members)
    padded = (rows + 2, width + 2, depth, members)
    face = (rows, width, members)
    f32 = jnp.float32
    dma = pltpu.SemaphoreType.DMA
    cells = rows * width * depth * members
    held = pl.pallas_call(
        functools.partial(kernel, rows, width, depth * zsize),
        out_shape=(pltpu.VMEM(block, f32), pltpu.VMEM(block, f32), pltpu.VMEM((2,) + face, f32), pltpu.VMEM(face, f32)),
        in_specs=[pl.BlockSpec(memory_space=pl.ANY)] * 3,
        out_specs=(pl.BlockSpec(memory_space=pltpu.VMEM),) * 4,
        scratch_shapes=[
            pltpu.VMEM(padded, f32),
            pltpu.VMEM(padded, f32),
            pltpu.VMEM(block, f32),
            pltpu.VMEM(block, f32),
            pltpu.VMEM((2, rows, 2, width, members), f32),
            pltpu.VMEM((2, rows, 2, width, members), f32),
            dma((5,)),
            dma((2,)),
            dma((4 + rows,)),
            dma((2,)),
            dma((2,)),
            dma((2,)),
            dma((2,)),
            dma((2,)),
            dma((2, rows)),
        ],
        compiler_params=pltpu.CompilerParams(
            collective_id=0, has_side_effects=True, vmem_limit_bytes=44 * 2**20
        ),
        cost_estimate=pl.CostEstimate(flops=48 * cells, bytes_accessed=20 * cells, transcendentals=0),
        name="diffuse",
    )(tracer, conductance, source)
    return pl.pallas_call(
        functools.partial(write_out, depth * zsize),
        out_shape=(jax.ShapeDtypeStruct(block, f32),) * 2,
        in_specs=[pl.BlockSpec(memory_space=pltpu.VMEM)] * 4,
        out_specs=(pl.BlockSpec(memory_space=pl.ANY),) * 2,
        scratch_shapes=[pltpu.VMEM(block, f32), dma((2,))],
        compiler_params=pltpu.CompilerParams(vmem_limit_bytes=10 * 2**20),
        cost_estimate=pl.CostEstimate(flops=cells, bytes_accessed=8 * cells, transcendentals=0),
        name="write_out",
    )(*held)


def solution(mesh):
    placed = P("py", "px", "pz", None)
    return jax.shard_map(
        on_device,
        mesh=mesh,
        in_specs=(placed, placed, placed),
        out_specs=(placed, placed),
        check_vma=False,
    )
```

```python
import functools

import jax
import jax.numpy as jnp
from jax import lax
from jax.experimental import pallas as pl
from jax.experimental.pallas import tpu as pltpu
from jax.sharding import PartitionSpec as P

MESH = pl.DeviceIdType.MESH
STEPS = 4
SLAB = 8
DOWN, UP = 0, 1

SHARES = {"chain": 5, "low": 3, "one": 2, "two": 2, "high": 3, "middle": 1}
ORIGINS = {
    "chain": ((UP, (0,)),),
    "two": ((DOWN, (2,)),),
    "one": ((DOWN, (1,)), (UP, (2,))),
    "low": ((UP, (1,)), (DOWN, (0,))),
    "high": ((UP, (0,)), (DOWN, (2,))),
    "middle": ((UP, (0, 2)), (DOWN, (1,))),
}
LATE_ORIGINS = {"two": ((UP, (0,)),)}
RELAYS = {
    "chain": ((UP, (1, 2), ()),),
    "two": ((DOWN, (1, 0), (3,)),),
    "one": ((DOWN, (0,), (3, 2)),),
    "low": ((UP, (2,), ()), (DOWN, (), (3, 2))),
    "high": ((UP, (1,), ()), (DOWN, (1, 0), ())),
    "middle": ((DOWN, (0,), (3,)),),
}
LAST = {
    (1, "one"): (DOWN, True),
    (1, "middle"): (UP, False),
    (1, "two"): (UP, False),
    (2, "high"): (UP, False),
    (2, "two"): (DOWN, True),
    (3, "chain"): (UP, False),
    (3, "high"): (DOWN, False),
}


def groups_of(rows):
    start, groups = 0, {}
    for kind, share in SHARES.items():
        groups[kind] = (start, start + share * rows // 16)
        start = groups[kind][1]
    return groups


def row_of(rows, i):
    half, odd_one = i // 2, i % 2
    return half + odd_one * (rows - 1 - 2 * half)


def on(mz, devices):
    hit = mz == devices[0]
    for device in devices[1:]:
        hit = jnp.logical_or(hit, mz == device)
    return pl.when(hit)


def add_below(out, base, p_in, y, ways, scale, own=None):
    def run(i, carry):
        for j in range(SLAB):
            x = i * SLAB + j
            below = p_in[ways[0], y, pl.ds(x, 1), :]
            for way in ways[1:]:
                below = below + p_in[way, y, pl.ds(x, 1), :]
            if own is not None:
                below = below - own[y, pl.ds(x, 1), :]
            out[x] = base[x] + below * scale
        return carry

    lax.fori_loop(0, base.shape[0] // SLAB, run, 0)


def kernel(
    rows, width, total_z,
    tracer, conductance, source,
    potential, end, p_in, total,
    even, odd, cond, src, z_out, z_in,
    load_sem, zs, zr, xs, xr, ys, yr, ps, pr,
):
    fields = (even, odd)
    axes = ("py", "px", "pz")
    me = {axis: lax.axis_index(axis) for axis in axes}
    near = {}
    for axis in axes:
        size = lax.axis_size(axis)
        near[axis] = (lax.rem(me[axis] + size - 1, size), lax.rem(me[axis] + 1, size))
    mz = me["pz"]
    last, quarter = rows - 1, rows // 4
    row_at = functools.partial(row_of, rows)

    parts = (((0, 1), (last, 1)), ((1, quarter - 1), (last - quarter + 1, quarter - 1)), ((quarter, 2 * quarter),))

    def rows_copy(start, size, sem):
        inside = even.at[pl.ds(1 + start, size), pl.ds(1, width)]
        return pltpu.make_async_copy(tracer.at[pl.ds(start, size)], inside, sem)

    def start_part(part):
        for start, size in parts[part]:
            rows_copy(start, size, load_sem.at[part]).start()

    def wait_part(part):
        rows_copy(0, sum(size for _, size in parts[part]), load_sem.at[part]).wait()

    def load_rest():
        return (
            pltpu.make_async_copy(conductance, cond, load_sem.at[3]),
            pltpu.make_async_copy(source, src, load_sem.at[4]),
        )

    def remote(a, b, send, recv, axis, way):
        return pltpu.make_async_remote_copy(
            src_ref=a, dst_ref=b, send_sem=send, recv_sem=recv,
            device_id={axis: near[axis][way]}, device_id_type=MESH,
        )

    def z_sem(par, y):
        index = turn_of(y)
        return zr.at[index // quarter] if par == 0 else zr.at[4 + index]

    def turn_of(y):
        far = y // (rows // 2)
        return 2 * (y + far * (last - 2 * y)) + far

    def z_copy(par, way, y):
        return remote(z_out.at[par, y, way], z_in.at[par, y, way], zs.at[par], z_sem(par, y), "pz", way)

    def z_all_sent(par):
        remote(z_out.at[par], z_in.at[par], zs.at[par], zr.at[0], "pz", UP).wait_send()

    def z_arrived(par, y):
        if par == 1:
            remote(z_out.at[par, y], z_in.at[par, y], zs.at[par], z_sem(par, y), "pz", UP).wait_recv()
            return
        group = pl.ds(0, quarter)

        @pl.when(turn_of(y) % quarter == 0)
        def _():
            remote(z_out.at[par, group], z_in.at[par, group], zs.at[par], z_sem(par, y), "pz", UP).wait_recv()

    def x_copy(par, way):
        field = fields[par]
        mine, theirs = ((1, width + 1), (width, 0))[way]
        inner = pl.ds(1, rows)
        return remote(field.at[inner, mine], field.at[inner, theirs], xs.at[par], xr.at[par], "px", way)

    def x_both(par):
        place = fields[par].at[pl.ds(1, rows), pl.ds(0, 2)]
        return remote(place, place, xs.at[par], xr.at[par], "px", UP)

    def y_copy(par, way):
        field = fields[par]
        mine, theirs = ((1, rows + 1), (rows, 0))[way]
        inner = pl.ds(1, width)
        return remote(field.at[mine, inner], field.at[theirs, inner], ys.at[par], yr.at[par], "py", way)

    def y_both(par):
        place = fields[par].at[pl.ds(0, 2), pl.ds(1, width)]
        return remote(place, place, ys.at[par], yr.at[par], "py", UP)

    def p_copy(way, y, place):
        return remote(place, p_in.at[way, y], ps.at[way], pr.at[way, y], "pz", way)

    def p_arrived(way, y):
        p_copy(way, y, total.at[y]).wait_recv()

    groups = groups_of(rows)

    def p_all_sent(way, device):
        count = sum(
            groups[kind][1] - groups[kind][0]
            for kind in SHARES
            for other, *devices in ORIGINS[kind] + LATE_ORIGINS.get(kind, ()) + RELAYS[kind]
            if other == way and device in sum(devices, ())
        )
        if count:

            @on(mz, (device,))
            def _():
                group = pl.ds(0, count)
                remote(total.at[group], p_in.at[way, group], ps.at[way], pr.at[way, 0], "pz", way).wait_send()

    def originate(origins, y):
        for way, devices in origins:

            @on(mz, devices)
            def _():
                p_copy(way, y, total.at[y]).start()

    def relay(kind, way, device, k):
        y = row_at(groups[kind][0] + k)
        adds = [pair[1] for pair in RELAYS[kind] if pair[0] == way][0]
        p_arrived(way, y)
        if device in adds:
            z_in[0, y, way] = p_in[way, y] + total[y]
            p_copy(way, y, z_in.at[0, y, way]).start()
        else:
            p_copy(way, y, p_in.at[way, y]).start()

    def conclude(kind, k, ways, waits=()):
        y = row_at(groups[kind][0] + k)
        for way in waits:
            p_arrived(way, y)
        add_below(potential.at[y], potential.at[y], p_in, y, ways, 1.0 / total_z)

    def send_row(par, y):
        for way in (DOWN, UP):
            z_copy(par, way, y).start()

        @pl.when(y == 0)
        def _():
            y_copy(par, DOWN).start()

        @pl.when(y == last)
        def _():
            y_copy(par, UP).start()

    def all_sent_of(par):
        z_all_sent(par)
        x_both(par).wait_send()
        y_both(par).wait_send()

    def arrived_row(par, y):
        @pl.when(y == 0)
        def _():
            y_both(par).wait_recv()

        z_arrived(par, y)

    def each_row(body):
        def run(i, carry):
            body(row_at(i))
            return carry

        lax.fori_loop(0, rows, run, 0)

    def each_slab(body):
        def run(i, carry):
            body(pl.multiple_of(i * SLAB, SLAB))
            return carry

        lax.fori_loop(0, width // SLAB, run, 0)

    barrier = pltpu.get_barrier_semaphore()
    for axis in ("pz", "px", "py"):
        for way in (DOWN, UP):
            pl.semaphore_signal(barrier, inc=1, device_id={axis: near[axis][way]}, device_id_type=MESH)

    for part in range(len(parts)):
        start_part(part)

    level = lax.broadcasted_iota(jnp.int32, (8, 128), 0)

    def pack(y):
        def slab(x0):
            for j in range(SLAB):
                value = even[1 + y, 1 + x0 + j]
                z_out[0, y, DOWN, pl.ds(x0 + j, 1), :] = value[0:1, :]
                z_out[0, y, UP, pl.ds(x0 + j, 1), :] = value[7:8, :]

        each_slab(slab)

    def some_rows(low, high, body):
        lax.fori_loop(low, high, lambda i, carry: (body(row_at(i)), carry)[1], 0)

    def first(y):
        pack(y)
        send_row(0, y)

    wait_part(0)
    some_rows(0, 2, pack)
    pl.semaphore_wait(barrier, 6)
    some_rows(0, 2, functools.partial(send_row, 0))
    wait_part(1)
    some_rows(2, 2 * quarter, first)
    wait_part(2)
    for copy in load_rest():
        copy.start()
    some_rows(2 * quarter, rows, first)
    for way in (DOWN, UP):
        x_copy(0, way).start()

    for step in range(1, STEPS + 1):
        old, new = (step - 1) % 2, step % 2
        before, after = fields[old], fields[new]
        if step == 1:
            for copy in load_rest():
                copy.wait()
        if 2 <= step < STEPS:
            all_sent_of(new)
        x_both(old).wait_recv()

        def advance(y, step=step, old=old, new=new, before=before, after=after):
            arrived_row(old, y)

            def slab(x0):
                line = [before[1 + y, x0 + j] for j in range(SLAB + 2)]
                for j in range(SLAB):
                    x = x0 + j
                    here = line[j + 1]
                    low = z_in[old, y, UP, pl.ds(x, 1), :]
                    high = z_in[old, y, DOWN, pl.ds(x, 1), :]
                    around = (line[j] + line[j + 2]) + (before[y, 1 + x] + before[2 + y, 1 + x])
                    below = pltpu.roll(jnp.where(level == 7, low, here), 1, 0)
                    above = pltpu.roll(jnp.where(level == 0, high, here), 7, 0)
                    spread = around + (below + above) - 6.0 * here
                    value = here + cond[y, x] * spread + src[y, x]
                    if step < STEPS:
                        after[1 + y, 1 + x] = value
                        z_out[new, y, DOWN, pl.ds(x, 1), :] = value[0:1, :]
                        z_out[new, y, UP, pl.ds(x, 1), :] = value[7:8, :]
                    else:
                        end[y, x] = value
                        run = value
                        for shift in (1, 2, 4):
                            run = run + jnp.where(level >= shift, pltpu.roll(run, shift, 0), 0.0)
                        potential[y, x] = run * (1.0 / total_z)
                        total[y, pl.ds(x, 1), :] = run[7:8, :]

            each_slab(slab)
            if step < STEPS:
                send_row(new, y)

        if step < STEPS:
            each_row(advance)
            for way in (DOWN, UP):
                x_copy(new, way).start()
            continue
        for kind, (low, high) in groups.items():

            def last_step(i, carry, kind=kind):
                y = row_at(i)
                advance(y)
                originate(ORIGINS[kind], y)
                return carry

            lax.fori_loop(low, high, last_step, 0)
        for kind, origins in LATE_ORIGINS.items():
            for i in range(*groups[kind]):
                originate(origins, row_at(i))

    def each(kind):
        return range(groups[kind][1] - groups[kind][0])

    @on(mz, (0,))
    def _():
        for kind in ("one", "middle", "two", "high"):
            for k in each(kind):
                relay(kind, DOWN, 0, k)

    @on(mz, (1,))
    def _():
        downs = [(kind, k) for kind in ("two", "high") for k in each(kind)]
        for k in each("chain"):
            relay("chain", UP, 1, k)
            if k < len(downs):
                relay(downs[k][0], DOWN, 1, downs[k][1])
        for k in each("chain"):
            conclude("chain", k, (UP,))
        for k in each("high"):
            relay("high", UP, 1, k)
            conclude("high", k, (UP,))
        for k in each("low"):
            conclude("low", k, (DOWN,), (DOWN,))

    @on(mz, (2,))
    def _():
        for k in each("low"):
            relay("low", UP, 2, k)
        downs = [(kind, k) for kind in ("low", "one") for k in each(kind)]
        for k in each("chain"):
            relay("chain", UP, 2, k)
            if k < len(downs):
                relay(downs[k][0], DOWN, 2, downs[k][1])
        for k in each("low"):
            conclude("low", k, (UP, DOWN))
        for k in each("chain"):
            conclude("chain", k, (UP,))
        for k in each("one"):
            conclude("one", k, (DOWN,))
        for k in each("middle"):
            conclude("middle", k, (DOWN,), (DOWN,))

    @on(mz, (3,))
    def _():
        for kind in ("low", "one", "middle", "two"):
            for k in each(kind):
                relay(kind, DOWN, 3, k)
        for kind in ("one", "middle", "low"):
            for k in each(kind):
                conclude(kind, k, (UP, DOWN), (UP,))
        for k in each("two"):
            conclude("two", k, (DOWN,))

    for (device, kind), (way, _) in LAST.items():

        @on(mz, (device,))
        def _():
            for i in range(*groups[kind]):
                p_arrived(way, row_at(i))

    for par in (0, 1):
        all_sent_of(par)
    for device in range(4):
        for way in (DOWN, UP):
            p_all_sent(way, device)


def write_out(total_z, held, end, p_in, total, potential_out, end_out, added, sem):
    mz = lax.axis_index("pz")
    rows = end.shape[0]
    quarter = rows // 4

    def potential_copy(y, source):
        return pltpu.make_async_copy(source, potential_out.at[y], sem.at[1])

    end_copy = pltpu.make_async_copy(end, end_out, sem.at[0])
    for place in range(4):
        part = pl.ds(place * quarter, quarter)
        pltpu.make_async_copy(end.at[part], end_out.at[part], sem.at[0]).start()
    for kind, (low, high) in groups_of(rows).items():
        late = [(device, *how) for (device, other), how in LAST.items() if other == kind]

        def run(i, carry, late=late):
            y = row_of(rows, i)
            plain = mz >= 0
            for device, way, off in late:
                plain = jnp.logical_and(plain, mz != device)

                @on(mz, (device,))
                def _():
                    own = total if off else None
                    add_below(added.at[i], held.at[y], p_in, y, (way,), 1.0 / total_z, own)
                    potential_copy(y, added.at[i]).start()

            @pl.when(plain)
            def _():
                potential_copy(y, held.at[y]).start()

            return carry

        lax.fori_loop(low, high, run, 0)
    pltpu.make_async_copy(held, potential_out, sem.at[1]).wait()
    end_copy.wait()


def on_device(tracer, conductance, source):
    rows, width, depth, members = tracer.shape
    zsize = lax.axis_size("pz")
    block = (rows, width, depth, members)
    padded = (rows + 2, width + 2, depth, members)
    face = (rows, width, members)
    f32 = jnp.float32
    dma = pltpu.SemaphoreType.DMA
    cells = rows * width * depth * members
    held = pl.pallas_call(
        functools.partial(kernel, rows, width, depth * zsize),
        out_shape=(pltpu.VMEM(block, f32), pltpu.VMEM(block, f32), pltpu.VMEM((2,) + face, f32), pltpu.VMEM(face, f32)),
        in_specs=[pl.BlockSpec(memory_space=pl.ANY)] * 3,
        out_specs=(pl.BlockSpec(memory_space=pltpu.VMEM),) * 4,
        scratch_shapes=[
            pltpu.VMEM(padded, f32),
            pltpu.VMEM(padded, f32),
            pltpu.VMEM(block, f32),
            pltpu.VMEM(block, f32),
            pltpu.VMEM((2, rows, 2, width, members), f32),
            pltpu.VMEM((2, rows, 2, width, members), f32),
            dma((5,)),
            dma((2,)),
            dma((4 + rows,)),
            dma((2,)),
            dma((2,)),
            dma((2,)),
            dma((2,)),
            dma((2,)),
            dma((2, rows)),
        ],
        compiler_params=pltpu.CompilerParams(
            collective_id=0, has_side_effects=True, vmem_limit_bytes=44 * 2**20
        ),
        cost_estimate=pl.CostEstimate(flops=48 * cells, bytes_accessed=20 * cells, transcendentals=0),
        name="diffuse",
    )(tracer, conductance, source)
    return pl.pallas_call(
        functools.partial(write_out, depth * zsize),
        out_shape=(jax.ShapeDtypeStruct(block, f32),) * 2,
        in_specs=[pl.BlockSpec(memory_space=pltpu.VMEM)] * 4,
        out_specs=(pl.BlockSpec(memory_space=pl.ANY),) * 2,
        scratch_shapes=[pltpu.VMEM(block, f32), dma((2,))],
        compiler_params=pltpu.CompilerParams(vmem_limit_bytes=10 * 2**20),
        cost_estimate=pl.CostEstimate(flops=cells, bytes_accessed=8 * cells, transcendentals=0),
        name="write_out",
    )(*held)


def solution(mesh):
    placed = P("py", "px", "pz", None)
    return jax.shard_map(
        on_device,
        mesh=mesh,
        in_specs=(placed, placed, placed),
        out_specs=(placed, placed),
        check_vma=False,
    )
```

```python
import functools

import jax
import jax.numpy as jnp
from jax import lax
from jax.experimental import pallas as pl
from jax.experimental.pallas import tpu as pltpu
from jax.sharding import PartitionSpec as P

MESH = pl.DeviceIdType.MESH
STEPS = 4
SLAB = 16
DOWN, UP = 0, 1

SHARES = {"chain": 5, "low": 3, "one": 2, "two": 2, "high": 3, "middle": 1}
ORIGINS = {
    "chain": ((UP, (0,)),),
    "two": ((DOWN, (2,)),),
    "one": ((DOWN, (1,)), (UP, (2,))),
    "low": ((UP, (1,)), (DOWN, (0,))),
    "high": ((UP, (0,)), (DOWN, (2,))),
    "middle": ((UP, (0, 2)), (DOWN, (1,))),
}
LATE_ORIGINS = {"two": ((UP, (0,)),)}
RELAYS = {
    "chain": ((UP, (1, 2), ()),),
    "two": ((DOWN, (1, 0), (3,)),),
    "one": ((DOWN, (0,), (3, 2)),),
    "low": ((UP, (2,), ()), (DOWN, (), (3, 2))),
    "high": ((UP, (1,), ()), (DOWN, (1, 0), ())),
    "middle": ((DOWN, (0,), (3,)),),
}
LAST = {
    (1, "one"): (DOWN, True),
    (1, "middle"): (UP, False),
    (1, "two"): (UP, False),
    (2, "high"): (UP, False),
    (2, "two"): (DOWN, True),
    (3, "chain"): (UP, False),
    (3, "high"): (DOWN, False),
}


def groups_of(rows):
    start, groups = 0, {}
    for kind, share in SHARES.items():
        groups[kind] = (start, start + share * rows // 16)
        start = groups[kind][1]
    return groups


def row_of(rows, i):
    half, odd_one = i // 2, i % 2
    return half + odd_one * (rows - 1 - 2 * half)


def on(mz, devices):
    hit = mz == devices[0]
    for device in devices[1:]:
        hit = jnp.logical_or(hit, mz == device)
    return pl.when(hit)


def add_below(out, base, p_in, y, ways, scale, own=None):
    def run(i, carry):
        for j in range(SLAB):
            x = i * SLAB + j
            below = p_in[ways[0], y, pl.ds(x, 1), :]
            for way in ways[1:]:
                below = below + p_in[way, y, pl.ds(x, 1), :]
            if own is not None:
                below = below - own[y, pl.ds(x, 1), :]
            out[x] = base[x] + below * scale
        return carry

    lax.fori_loop(0, base.shape[0] // SLAB, run, 0)


def kernel(
    rows, width, total_z,
    tracer, conductance, source,
    potential, end, p_in, total,
    even, odd, cond, src, z_out, z_in,
    load_sem, zs, zr, xs, xr, ys, yr, ps, pr,
):
    fields = (even, odd)
    axes = ("py", "px", "pz")
    me = {axis: lax.axis_index(axis) for axis in axes}
    near = {}
    for axis in axes:
        size = lax.axis_size(axis)
        near[axis] = (lax.rem(me[axis] + size - 1, size), lax.rem(me[axis] + 1, size))
    mz = me["pz"]
    last, quarter = rows - 1, rows // 4
    row_at = functools.partial(row_of, rows)

    parts = (((0, 1), (last, 1)), ((1, quarter - 1), (last - quarter + 1, quarter - 1)), ((quarter, 2 * quarter),))

    def rows_copy(start, size, sem):
        inside = even.at[pl.ds(1 + start, size), pl.ds(1, width)]
        return pltpu.make_async_copy(tracer.at[pl.ds(start, size)], inside, sem)

    def start_part(part):
        for start, size in parts[part]:
            rows_copy(start, size, load_sem.at[part]).start()

    def wait_part(part):
        rows_copy(0, sum(size for _, size in parts[part]), load_sem.at[part]).wait()

    def load_rest():
        return (
            pltpu.make_async_copy(conductance, cond, load_sem.at[3]),
            pltpu.make_async_copy(source, src, load_sem.at[4]),
        )

    def remote(a, b, send, recv, axis, way):
        return pltpu.make_async_remote_copy(
            src_ref=a, dst_ref=b, send_sem=send, recv_sem=recv,
            device_id={axis: near[axis][way]}, device_id_type=MESH,
        )

    def z_sem(par, y):
        index = turn_of(y)
        return zr.at[index // quarter] if par == 0 else zr.at[4 + index]

    def turn_of(y):
        far = y // (rows // 2)
        return 2 * (y + far * (last - 2 * y)) + far

    def z_copy(par, way, y):
        return remote(z_out.at[par, y, way], z_in.at[par, y, way], zs.at[par], z_sem(par, y), "pz", way)

    def z_all_sent(par):
        remote(z_out.at[par], z_in.at[par], zs.at[par], zr.at[0], "pz", UP).wait_send()

    def z_arrived(par, y):
        if par == 1:
            remote(z_out.at[par, y], z_in.at[par, y], zs.at[par], z_sem(par, y), "pz", UP).wait_recv()
            return
        group = pl.ds(0, quarter)

        @pl.when(turn_of(y) % quarter == 0)
        def _():
            remote(z_out.at[par, group], z_in.at[par, group], zs.at[par], z_sem(par, y), "pz", UP).wait_recv()

    def x_copy(par, way):
        field = fields[par]
        mine, theirs = ((1, width + 1), (width, 0))[way]
        inner = pl.ds(1, rows)
        return remote(field.at[inner, mine], field.at[inner, theirs], xs.at[par], xr.at[par], "px", way)

    def x_both(par):
        place = fields[par].at[pl.ds(1, rows), pl.ds(0, 2)]
        return remote(place, place, xs.at[par], xr.at[par], "px", UP)

    def y_copy(par, way):
        field = fields[par]
        mine, theirs = ((1, rows + 1), (rows, 0))[way]
        inner = pl.ds(1, width)
        return remote(field.at[mine, inner], field.at[theirs, inner], ys.at[par], yr.at[par], "py", way)

    def y_both(par):
        place = fields[par].at[pl.ds(0, 2), pl.ds(1, width)]
        return remote(place, place, ys.at[par], yr.at[par], "py", UP)

    def p_copy(way, y, place):
        return remote(place, p_in.at[way, y], ps.at[way], pr.at[way, y], "pz", way)

    def p_arrived(way, y):
        p_copy(way, y, total.at[y]).wait_recv()

    groups = groups_of(rows)

    def p_all_sent(way, device):
        count = sum(
            groups[kind][1] - groups[kind][0]
            for kind in SHARES
            for other, *devices in ORIGINS[kind] + LATE_ORIGINS.get(kind, ()) + RELAYS[kind]
            if other == way and device in sum(devices, ())
        )
        if count:

            @on(mz, (device,))
            def _():
                group = pl.ds(0, count)
                remote(total.at[group], p_in.at[way, group], ps.at[way], pr.at[way, 0], "pz", way).wait_send()

    def originate(origins, y):
        for way, devices in origins:

            @on(mz, devices)
            def _():
                p_copy(way, y, total.at[y]).start()

    def relay(kind, way, device, k):
        y = row_at(groups[kind][0] + k)
        adds = [pair[1] for pair in RELAYS[kind] if pair[0] == way][0]
        p_arrived(way, y)
        if device in adds:
            z_in[0, y, way] = p_in[way, y] + total[y]
            p_copy(way, y, z_in.at[0, y, way]).start()
        else:
            p_copy(way, y, p_in.at[way, y]).start()

    def conclude(kind, k, ways, waits=()):
        y = row_at(groups[kind][0] + k)
        for way in waits:
            p_arrived(way, y)
        add_below(potential.at[y], potential.at[y], p_in, y, ways, 1.0 / total_z)

    def send_row(par, y):
        for way in (DOWN, UP):
            z_copy(par, way, y).start()

        @pl.when(y == 0)
        def _():
            y_copy(par, DOWN).start()

        @pl.when(y == last)
        def _():
            y_copy(par, UP).start()

    def all_sent_of(par):
        z_all_sent(par)
        x_both(par).wait_send()
        y_both(par).wait_send()

    def arrived_row(par, y):
        @pl.when(y == 0)
        def _():
            y_both(par).wait_recv()

        z_arrived(par, y)

    def each_row(body):
        def run(i, carry):
            body(row_at(i))
            return carry

        lax.fori_loop(0, rows, run, 0)

    def each_slab(body):
        def run(i, carry):
            body(pl.multiple_of(i * SLAB, SLAB))
            return carry

        lax.fori_loop(0, width // SLAB, run, 0)

    barrier = pltpu.get_barrier_semaphore()
    for axis in ("pz", "px", "py"):
        for way in (DOWN, UP):
            pl.semaphore_signal(barrier, inc=1, device_id={axis: near[axis][way]}, device_id_type=MESH)

    for part in range(len(parts)):
        start_part(part)

    level = lax.broadcasted_iota(jnp.int32, (8, 128), 0)

    def pack(y):
        def slab(x0):
            for j in range(SLAB):
                value = even[1 + y, 1 + x0 + j]
                z_out[0, y, DOWN, pl.ds(x0 + j, 1), :] = value[0:1, :]
                z_out[0, y, UP, pl.ds(x0 + j, 1), :] = value[7:8, :]

        each_slab(slab)

    def some_rows(low, high, body):
        lax.fori_loop(low, high, lambda i, carry: (body(row_at(i)), carry)[1], 0)

    def first(y):
        pack(y)
        send_row(0, y)

    wait_part(0)
    some_rows(0, 2, pack)
    pl.semaphore_wait(barrier, 6)
    some_rows(0, 2, functools.partial(send_row, 0))
    wait_part(1)
    some_rows(2, 2 * quarter, first)
    wait_part(2)
    for copy in load_rest():
        copy.start()
    some_rows(2 * quarter, rows, first)
    for way in (DOWN, UP):
        x_copy(0, way).start()

    for step in range(1, STEPS + 1):
        old, new = (step - 1) % 2, step % 2
        before, after = fields[old], fields[new]
        if step == 1:
            for copy in load_rest():
                copy.wait()
        if 2 <= step < STEPS:
            all_sent_of(new)
        x_both(old).wait_recv()

        def advance(y, step=step, old=old, new=new, before=before, after=after):
            arrived_row(old, y)

            def slab(x0):
                line = [before[1 + y, x0 + j] for j in range(SLAB + 2)]
                for j in range(SLAB):
                    x = x0 + j
                    here = line[j + 1]
                    low = z_in[old, y, UP, pl.ds(x, 1), :]
                    high = z_in[old, y, DOWN, pl.ds(x, 1), :]
                    around = (line[j] + line[j + 2]) + (before[y, 1 + x] + before[2 + y, 1 + x])
                    below = pltpu.roll(jnp.where(level == 7, low, here), 1, 0)
                    above = pltpu.roll(jnp.where(level == 0, high, here), 7, 0)
                    spread = around + (below + above) - 6.0 * here
                    value = here + cond[y, x] * spread + src[y, x]
                    if step < STEPS:
                        after[1 + y, 1 + x] = value
                        z_out[new, y, DOWN, pl.ds(x, 1), :] = value[0:1, :]
                        z_out[new, y, UP, pl.ds(x, 1), :] = value[7:8, :]
                    else:
                        end[y, x] = value
                        run = value
                        for shift in (1, 2, 4):
                            run = run + jnp.where(level >= shift, pltpu.roll(run, shift, 0), 0.0)
                        potential[y, x] = run * (1.0 / total_z)
                        total[y, pl.ds(x, 1), :] = run[7:8, :]

            each_slab(slab)
            if step < STEPS:
                send_row(new, y)

        if step < STEPS:
            each_row(advance)
            for way in (DOWN, UP):
                x_copy(new, way).start()
            continue
        for kind, (low, high) in groups.items():

            def last_step(i, carry, kind=kind):
                y = row_at(i)
                advance(y)
                originate(ORIGINS[kind], y)
                return carry

            lax.fori_loop(low, high, last_step, 0)
        for kind, origins in LATE_ORIGINS.items():
            for i in range(*groups[kind]):
                originate(origins, row_at(i))

    def each(kind):
        return range(groups[kind][1] - groups[kind][0])

    @on(mz, (0,))
    def _():
        for kind in ("one", "middle", "two", "high"):
            for k in each(kind):
                relay(kind, DOWN, 0, k)

    @on(mz, (1,))
    def _():
        downs = [(kind, k) for kind in ("two", "high") for k in each(kind)]
        for k in each("chain"):
            relay("chain", UP, 1, k)
            if k < len(downs):
                relay(downs[k][0], DOWN, 1, downs[k][1])
        for k in each("chain"):
            conclude("chain", k, (UP,))
        for k in each("high"):
            relay("high", UP, 1, k)
            conclude("high", k, (UP,))
        for k in each("low"):
            conclude("low", k, (DOWN,), (DOWN,))

    @on(mz, (2,))
    def _():
        for k in each("low"):
            relay("low", UP, 2, k)
        downs = [(kind, k) for kind in ("low", "one") for k in each(kind)]
        for k in each("chain"):
            relay("chain", UP, 2, k)
            if k < len(downs):
                relay(downs[k][0], DOWN, 2, downs[k][1])
        for k in each("low"):
            conclude("low", k, (UP, DOWN))
        for k in each("chain"):
            conclude("chain", k, (UP,))
        for k in each("one"):
            conclude("one", k, (DOWN,))
        for k in each("middle"):
            conclude("middle", k, (DOWN,), (DOWN,))

    @on(mz, (3,))
    def _():
        for kind in ("low", "one", "middle", "two"):
            for k in each(kind):
                relay(kind, DOWN, 3, k)
        for kind in ("one", "middle", "low"):
            for k in each(kind):
                conclude(kind, k, (UP, DOWN), (UP,))
        for k in each("two"):
            conclude("two", k, (DOWN,))

    for (device, kind), (way, _) in LAST.items():

        @on(mz, (device,))
        def _():
            for i in range(*groups[kind]):
                p_arrived(way, row_at(i))

    for par in (0, 1):
        all_sent_of(par)
    for device in range(4):
        for way in (DOWN, UP):
            p_all_sent(way, device)


def write_out(total_z, held, end, p_in, total, potential_out, end_out, added, sem):
    mz = lax.axis_index("pz")
    rows = end.shape[0]
    quarter = rows // 4

    def potential_copy(y, source):
        return pltpu.make_async_copy(source, potential_out.at[y], sem.at[1])

    end_copy = pltpu.make_async_copy(end, end_out, sem.at[0])
    for place in range(4):
        part = pl.ds(place * quarter, quarter)
        pltpu.make_async_copy(end.at[part], end_out.at[part], sem.at[0]).start()
    for kind, (low, high) in groups_of(rows).items():
        late = [(device, *how) for (device, other), how in LAST.items() if other == kind]

        def run(i, carry, late=late):
            y = row_of(rows, i)
            plain = mz >= 0
            for device, way, off in late:
                plain = jnp.logical_and(plain, mz != device)

                @on(mz, (device,))
                def _():
                    own = total if off else None
                    add_below(added.at[i], held.at[y], p_in, y, (way,), 1.0 / total_z, own)
                    potential_copy(y, added.at[i]).start()

            @pl.when(plain)
            def _():
                potential_copy(y, held.at[y]).start()

            return carry

        lax.fori_loop(low, high, run, 0)
    pltpu.make_async_copy(held, potential_out, sem.at[1]).wait()
    end_copy.wait()


def on_device(tracer, conductance, source):
    rows, width, depth, members = tracer.shape
    zsize = lax.axis_size("pz")
    block = (rows, width, depth, members)
    padded = (rows + 2, width + 2, depth, members)
    face = (rows, width, members)
    f32 = jnp.float32
    dma = pltpu.SemaphoreType.DMA
    cells = rows * width * depth * members
    held = pl.pallas_call(
        functools.partial(kernel, rows, width, depth * zsize),
        out_shape=(pltpu.VMEM(block, f32), pltpu.VMEM(block, f32), pltpu.VMEM((2,) + face, f32), pltpu.VMEM(face, f32)),
        in_specs=[pl.BlockSpec(memory_space=pl.ANY)] * 3,
        out_specs=(pl.BlockSpec(memory_space=pltpu.VMEM),) * 4,
        scratch_shapes=[
            pltpu.VMEM(padded, f32),
            pltpu.VMEM(padded, f32),
            pltpu.VMEM(block, f32),
            pltpu.VMEM(block, f32),
            pltpu.VMEM((2, rows, 2, width, members), f32),
            pltpu.VMEM((2, rows, 2, width, members), f32),
            dma((5,)),
            dma((2,)),
            dma((4 + rows,)),
            dma((2,)),
            dma((2,)),
            dma((2,)),
            dma((2,)),
            dma((2,)),
            dma((2, rows)),
        ],
        compiler_params=pltpu.CompilerParams(
            collective_id=0, has_side_effects=True, vmem_limit_bytes=44 * 2**20
        ),
        cost_estimate=pl.CostEstimate(flops=48 * cells, bytes_accessed=20 * cells, transcendentals=0),
        name="diffuse",
    )(tracer, conductance, source)
    return pl.pallas_call(
        functools.partial(write_out, depth * zsize),
        out_shape=(jax.ShapeDtypeStruct(block, f32),) * 2,
        in_specs=[pl.BlockSpec(memory_space=pltpu.VMEM)] * 4,
        out_specs=(pl.BlockSpec(memory_space=pl.ANY),) * 2,
        scratch_shapes=[pltpu.VMEM(block, f32), dma((2,))],
        compiler_params=pltpu.CompilerParams(vmem_limit_bytes=10 * 2**20),
        cost_estimate=pl.CostEstimate(flops=cells, bytes_accessed=8 * cells, transcendentals=0),
        name="write_out",
    )(*held)


def solution(mesh):
    placed = P("py", "px", "pz", None)
    return jax.shard_map(
        on_device,
        mesh=mesh,
        in_specs=(placed, placed, placed),
        out_specs=(placed, placed),
        check_vma=False,
    )
```
